8 devices in a mesh: depth: 2 (over z, y), col: 2 (over x), row: 2 (over core).
Axes of the slice: x: 2, y: 2, z: 1, core: 2. Of those that a mesh axis runs over, the one named last changes fastest.
Arguments:
- a_mat: bfloat16 [4096, 4096], P('row', 'col')
- b_mat: bfloat16 [4096, 4096], P('row', 'col')
Outputs:
- output: bfloat16 [4096, 4096], P(('row', 'depth'), 'col')
All inputs are finite; a program needn't handle non-finite values.
Results may differ from the reference program's by a relative error of at most 0.001.
Values are sent between devices in bfloat16 or wider.
A program may use at most 1 GiB of HBM per device.

```python
import jax
import jax.numpy as jnp

D = 4096


def setup_inputs(seed: int = 0) -> dict:
    key_a, key_b = jax.random.split(jax.random.key(seed))
    a_mat = jax.random.normal(key_a, (D, D), jnp.float32) + 0.5
    b_mat = (jax.random.normal(key_b, (D, D), jnp.float32) + 2.0 * D ** -0.5) * D ** -0.5
    return {"a_mat": a_mat.astype(jnp.bfloat16), "b_mat": b_mat.astype(jnp.bfloat16)}


def reference(a_mat, b_mat):
    return jnp.dot(a_mat, b_mat, preferred_element_type=jnp.float32).astype(jnp.bfloat16)
```

```python
import functools

import jax
import jax.numpy as jnp
from jax import lax
from jax.experimental import pallas as pl
from jax.experimental.pallas import tpu as pltpu
from jax.sharding import PartitionSpec as P

MESH = pl.DeviceIdType.MESH
CHUNKS = (256, 256, 256, 128, 64, 64)
B_PARTS = 4
TILE_M = 256
TILE_N = 256


def kernel(a_ref, b_ref, c_ref, a_own, a_far, b_buf, total, own_sem, bown_sem, bsend_sem, brecv_sem, asend_sem, arecv_sem):
    layer, col, row = lax.axis_index("depth"), lax.axis_index("col"), lax.axis_index("row")
    rows = c_ref.shape[0]
    depth, cols = b_ref.shape
    across = (layer, 1 - col, row)
    beside = (layer, col, 1 - row)
    base = layer * rows
    slot = lax.rem(row + col, 2)

    own_a = pltpu.make_async_copy(a_ref.at[pl.ds(base, rows), :], a_own, own_sem)
    own_b = pltpu.make_async_copy(b_ref, b_buf.at[slot], bown_sem)
    own_a.start()
    own_b.start()

    barrier = pltpu.get_barrier_semaphore()
    for peer in (across, beside):
        pl.semaphore_signal(barrier, inc=1, device_id=peer, device_id_type=MESH)
    pl.semaphore_wait(barrier, 2)

    a_sends = []
    start = 0
    for idx, size in enumerate(CHUNKS):
        a_sends.append(
            pltpu.make_async_remote_copy(
                src_ref=a_ref.at[pl.ds(base + start, size), :],
                dst_ref=a_far.at[pl.ds(start, size), :],
                send_sem=asend_sem.at[idx],
                recv_sem=arecv_sem.at[idx],
                device_id=across,
                device_id_type=MESH,
            )
        )
        start += size
    b_sends = []
    part = depth // B_PARTS
    for idx in range(B_PARTS):
        b_sends.append(
            pltpu.make_async_remote_copy(
                src_ref=b_ref.at[pl.ds(idx * part, part), :],
                dst_ref=b_buf.at[slot, pl.ds(idx * part, part), :],
                send_sem=bsend_sem.at[idx],
                recv_sem=brecv_sem.at[idx],
                device_id=beside,
                device_id_type=MESH,
            )
        )
    a_sends[0].start()
    for send in b_sends:
        send.start()
    for send in a_sends[1:]:
        send.start()

    own_a.wait()
    own_b.wait()
    for send in b_sends:
        send.wait_recv()

    col_tiles = cols // TILE_N

    @pl.loop(0, (rows // TILE_M) * col_tiles)
    def _(tile):
        r = pl.ds(pl.multiple_of((tile // col_tiles) * TILE_M, TILE_M), TILE_M)
        c = pl.ds(pl.multiple_of((tile % col_tiles) * TILE_N, TILE_N), TILE_N)
        total[r, c] = jnp.dot(a_own[r, :], b_buf[0, :, c], preferred_element_type=jnp.float32)

    start = 0
    for idx, size in enumerate(CHUNKS):
        a_sends[idx].wait_recv()
        r = pl.ds(start, size)

        @pl.loop(0, col_tiles)
        def _(tile):
            c = pl.ds(pl.multiple_of(tile * TILE_N, TILE_N), TILE_N)
            rest = jnp.dot(a_far[r, :], b_buf[1, :, c], preferred_element_type=jnp.float32)
            c_ref[r, c] = (total[r, c] + rest).astype(c_ref.dtype)

        start += size

    for send in a_sends + b_sends:
        send.wait_send()


def solution(mesh):
    depth_n = mesh.shape["depth"]

    def local_mm(a_blk, b_blk):
        rows = a_blk.shape[0] // depth_n
        depth, cols = b_blk.shape
        n = len(CHUNKS)
        dma = pltpu.SemaphoreType.DMA
        return pl.pallas_call(
            kernel,
            out_shape=jax.ShapeDtypeStruct((rows, cols), jnp.bfloat16),
            in_specs=[pl.BlockSpec(memory_space=pl.ANY)] * 2,
            out_specs=pl.BlockSpec(memory_space=pltpu.VMEM),
            scratch_shapes=[
                pltpu.VMEM((rows, depth), jnp.bfloat16),
                pltpu.VMEM((rows, depth), jnp.bfloat16),
                pltpu.VMEM((2, depth, cols), jnp.bfloat16),
                pltpu.VMEM((rows, cols), jnp.float32),
                dma,
                dma,
                dma((B_PARTS,)),
                dma((B_PARTS,)),
                dma((n,)),
                dma((n,)),
            ],
            compiler_params=pltpu.CompilerParams(
                collective_id=0, has_side_effects=True, vmem_limit_bytes=56 * 1024 * 1024
            ),
            cost_estimate=pl.CostEstimate(flops=4 * rows * depth * cols, bytes_accessed=2 * (6 * depth * cols), transcendentals=0),
        )(a_blk, b_blk)

    return jax.shard_map(
        local_mm, mesh=mesh, in_specs=(P("row", "col"), P("row", "col")), out_specs=P(("row", "depth"), "col"), check_vma=False
    )
```

```python
import jax
import jax.numpy as jnp
from jax import lax
from jax.experimental import pallas as pl
from jax.experimental.pallas import tpu as pltpu
from jax.sharding import PartitionSpec as P

MESH = pl.DeviceIdType.MESH
PIECES = (
    (0, 256, 0, 2048, 8, False),
    (256, 256, 0, 2048, 8, False),
    (512, 256, 0, 2048, 8, False),
    (768, 256, 0, 1024, 8, False),
    (768, 256, 1024, 512, 8, False),
    (768, 256, 1536, 256, 4, True),
    (768, 256, 1792, 256, 4, True),
)
B_PARTS = 4
TILE_M = 256
TILE_N = 256


def kernel(a_ref, b_ref, c_ref, a_own, a_far, b_buf, total, own_sem, bown_sem, bsend_sem, brecv_sem, asend_sem, arecv_sem, ready_sem):
    layer, col, row = lax.axis_index("depth"), lax.axis_index("col"), lax.axis_index("row")
    rows = c_ref.shape[0]
    depth, cols = b_ref.shape
    across = (layer, 1 - col, row)
    beside = (layer, col, 1 - row)
    base = layer * rows
    slot = lax.rem(row + col, 2)

    barrier = pltpu.get_barrier_semaphore()
    pl.semaphore_signal(barrier, inc=1, device_id=across, device_id_type=MESH)

    @pl.when(row == 1)
    def _():
        pl.semaphore_signal(barrier, inc=1, device_id=beside, device_id_type=MESH)
        pl.semaphore_wait(barrier, 1)

    @pl.when(row == 0)
    def _():
        pl.semaphore_wait(barrier, 2)
        pl.semaphore_signal(ready_sem, inc=1, device_id=beside, device_id_type=MESH)

    a_sends = []
    for idx, (r0, nr, k0, nk, _, _) in enumerate(PIECES):
        a_sends.append(
            pltpu.make_async_remote_copy(
                src_ref=a_ref.at[pl.ds(base + r0, nr), pl.ds(k0, nk)],
                dst_ref=a_far.at[pl.ds(r0, nr), pl.ds(k0, nk)],
                send_sem=asend_sem.at[idx],
                recv_sem=arecv_sem.at[idx],
                device_id=across,
                device_id_type=MESH,
            )
        )
    b_sends = []
    part = depth // B_PARTS
    for idx in range(B_PARTS):
        b_sends.append(
            pltpu.make_async_remote_copy(
                src_ref=b_ref.at[pl.ds(idx * part, part), :],
                dst_ref=b_buf.at[slot, pl.ds(idx * part, part), :],
                send_sem=bsend_sem.at[idx],
                recv_sem=brecv_sem.at[idx],
                device_id=beside,
                device_id_type=MESH,
            )
        )
    own_a = pltpu.make_async_copy(a_ref.at[pl.ds(base, rows), :], a_own, own_sem)
    own_b = pltpu.make_async_copy(b_ref, b_buf.at[slot], bown_sem)

    a_sends[0].start()

    @pl.when(row == 1)
    def _():
        pl.semaphore_wait(ready_sem, 1)

    for send in b_sends:
        send.start()
    for send in a_sends[1:]:
        send.start()
    own_a.start()
    own_b.start()
    own_a.wait()
    own_b.wait()
    for send in b_sends:
        send.wait_recv()

    col_tiles = cols // TILE_N

    @pl.loop(0, (rows // TILE_M) * col_tiles)
    def _(tile):
        r = pl.ds(pl.multiple_of((tile // col_tiles) * TILE_M, TILE_M), TILE_M)
        c = pl.ds(pl.multiple_of((tile % col_tiles) * TILE_N, TILE_N), TILE_N)
        total[r, c] = jnp.dot(a_own[r, :], b_buf[0, :, c], preferred_element_type=jnp.float32)

    for idx, (r0, nr, k0, nk, tiles, unroll) in enumerate(PIECES):
        a_sends[idx].wait_recv()
        r, k, tn = pl.ds(r0, nr), pl.ds(k0, nk), cols // tiles

        def add(c):
            sums = total[r, c] + jnp.dot(a_far[r, k], b_buf[1, k, c], preferred_element_type=jnp.float32)
            if k0 + nk == depth:
                c_ref[r, c] = sums.astype(c_ref.dtype)
            else:
                total[r, c] = sums

        if unroll:
            for tile in range(tiles):
                add(pl.ds(tile * tn, tn))
        else:

            @pl.loop(0, tiles)
            def _(tile):
                add(pl.ds(pl.multiple_of(tile * tn, tn), tn))

    for send in a_sends + b_sends:
        send.wait_send()


def solution(mesh):
    depth_n = mesh.shape["depth"]

    def local_mm(a_blk, b_blk):
        rows = a_blk.shape[0] // depth_n
        depth, cols = b_blk.shape
        n = len(PIECES)
        dma = pltpu.SemaphoreType.DMA
        return pl.pallas_call(
            kernel,
            out_shape=pltpu.VMEM((rows, cols), jnp.bfloat16),
            in_specs=[pl.BlockSpec(memory_space=pl.ANY)] * 2,
            out_specs=pl.BlockSpec(memory_space=pltpu.VMEM),
            scratch_shapes=[
                pltpu.VMEM((rows, depth), jnp.bfloat16),
                pltpu.VMEM((rows, depth), jnp.bfloat16),
                pltpu.VMEM((2, depth, cols), jnp.bfloat16),
                pltpu.VMEM((rows, cols), jnp.float32),
                dma,
                dma,
                dma((B_PARTS,)),
                dma((B_PARTS,)),
                dma((n,)),
                dma((n,)),
                pltpu.SemaphoreType.REGULAR,
            ],
            compiler_params=pltpu.CompilerParams(
                collective_id=0, has_side_effects=True, vmem_limit_bytes=56 * 1024 * 1024
            ),
            cost_estimate=pl.CostEstimate(flops=4 * rows * depth * cols, bytes_accessed=12 * depth * cols, transcendentals=0),
        )(a_blk, b_blk)

    return jax.shard_map(
        local_mm, mesh=mesh, in_specs=(P("row", "col"), P("row", "col")), out_specs=P(("row", "depth"), "col"), check_vma=False
    )
```

```python
import functools

import jax
import jax.numpy as jnp
from jax import lax
from jax.experimental import pallas as pl
from jax.experimental.pallas import tpu as pltpu
from jax.sharding import PartitionSpec as P

MESH = pl.DeviceIdType.MESH
BOTTOM = 192
FIRST = (
    (0, 256, 0, 2048),
    (256, 256, 0, 2048),
    (512, 128, 0, 2048),
    (640, 64, 0, 2048),
    (704, 128, 0, 512),
    (704, 128, 512, 512),
    (704, 128, 1024, 512),
    (704, 128, 1536, 512),
)
SECOND = (
    (0, 192, 0, 1024),
    (0, 192, 1024, 512),
    (0, 192, 1536, 256),
    (0, 192, 1792, 256),
)
HOLD = 3
TURN = 4
B_PARTS = 4
TILE_M = 256
TILE_N = 256


def place():
    layer, col, row = lax.axis_index("depth"), lax.axis_index("col"), lax.axis_index("row")
    return layer, row, (layer, 1 - col, row), (layer, col, 1 - row), lax.rem(row + col, 2)


def sends_of(pieces, a_ref, first_row, a_far, send_sem, recv_sem, device):
    return [
        pltpu.make_async_remote_copy(
            src_ref=a_ref.at[pl.ds(first_row + r0, nr), pl.ds(k0, nk)],
            dst_ref=a_far.at[pl.ds(r0, nr), pl.ds(k0, nk)],
            send_sem=send_sem.at[idx],
            recv_sem=recv_sem.at[idx],
            device_id=device,
            device_id_type=MESH,
        )
        for idx, (r0, nr, k0, nk) in enumerate(pieces)
    ]


def multiply(piece, a_far, b_far, total, c_ref):
    r0, nr, k0, nk = piece
    depth, cols = b_far.shape
    r, k = pl.ds(r0, nr), pl.ds(k0, nk)

    def add(c):
        sums = total[r, c] + jnp.dot(a_far[r, k], b_far[k, c], preferred_element_type=jnp.float32)
        if k0 + nk == depth:
            c_ref[r, c] = sums.astype(c_ref.dtype)
        else:
            total[r, c] = sums

    if nk <= 512:
        for tile in range(4):
            add(pl.ds(tile * (cols // 4), cols // 4))
    else:

        @pl.loop(0, cols // TILE_N)
        def _(tile):
            add(pl.ds(pl.multiple_of(tile * TILE_N, TILE_N), TILE_N))


def first_kernel(
    a_ref, b_ref, c_ref, b_far, low, a_own, a_far, b_near, total, own_sem, bown_sem, bsend_sem, brecv_sem, asend_sem, arecv_sem, ready_sem, turn_sem
):
    layer, row, across, beside, slot = place()
    top, cols = c_ref.shape
    rows, depth = a_own.shape
    base = layer * rows

    barrier = pltpu.get_barrier_semaphore()
    pl.semaphore_signal(barrier, inc=1, device_id=across, device_id_type=MESH)

    @pl.when(row == 1)
    def _():
        pl.semaphore_signal(barrier, inc=1, device_id=beside, device_id_type=MESH)
        pl.semaphore_wait(barrier, 1)

    @pl.when(row == 0)
    def _():
        pl.semaphore_wait(barrier, 2)
        pl.semaphore_signal(ready_sem, inc=1, device_id=beside, device_id_type=MESH)

    a_sends = sends_of(FIRST, a_ref, base, a_far, asend_sem, arecv_sem, across)
    part = depth // B_PARTS

    def sends_of_b(b_buf):
        return [
            pltpu.make_async_remote_copy(
                src_ref=b_ref.at[pl.ds(idx * part, part), :],
                dst_ref=b_buf.at[pl.ds(idx * part, part), :],
                send_sem=bsend_sem.at[idx],
                recv_sem=brecv_sem.at[idx],
                device_id=beside,
                device_id_type=MESH,
            )
            for idx in range(B_PARTS)
        ]

    def own_of_b(b_buf):
        return pltpu.make_async_copy(b_ref, b_buf, bown_sem)

    own_a = pltpu.make_async_copy(a_ref.at[pl.ds(base, rows), :], a_own, own_sem)

    a_sends[0].start()

    @pl.when(row == 1)
    def _():
        pl.semaphore_wait(ready_sem, 1)

    for value, b_buf in enumerate((b_near, b_far)):

        @pl.when(slot == value)
        def _():
            for send in sends_of_b(b_buf):
                send.start()

    for send in a_sends[1:HOLD]:
        send.start()

    @pl.when(row == 0)
    def _():
        for send in a_sends[HOLD:]:
            send.start()

    own_a.start()
    for value, b_buf in enumerate((b_near, b_far)):

        @pl.when(slot == value)
        def _():
            own_of_b(b_buf).start()

    own_a.wait()
    for value, (b_mine, b_other) in enumerate(((b_near, b_far), (b_far, b_near))):

        @pl.when(slot == value)
        def _():
            own_of_b(b_mine).wait()
            for send in sends_of_b(b_other):
                send.wait_recv()


    col_tiles = cols // TILE_N

    tile_m = top // 4

    @pl.loop(0, 4 * col_tiles)
    def _(tile):
        r = pl.ds(pl.multiple_of((tile // col_tiles) * tile_m, 16), tile_m)
        c = pl.ds(pl.multiple_of((tile % col_tiles) * TILE_N, TILE_N), TILE_N)
        total[r, c] = jnp.dot(a_own[r, :], b_near[:, c], preferred_element_type=jnp.float32)

    @pl.loop(0, col_tiles)
    def _(tile):
        c = pl.ds(pl.multiple_of(tile * TILE_N, TILE_N), TILE_N)
        low[:, c] = jnp.dot(a_own[pl.ds(top, rows - top), :], b_near[:, c], preferred_element_type=jnp.float32)

    for idx, piece in enumerate(FIRST):
        if idx == HOLD:

            @pl.when(row == 1)
            def _():
                pl.semaphore_wait(turn_sem, 1)
                for send in a_sends[HOLD:]:
                    send.start()

        a_sends[idx].wait_recv()
        if idx == TURN:

            @pl.when(row == 0)
            def _():
                a_sends[TURN].wait_send()
                pl.semaphore_signal(turn_sem, inc=1, device_id=beside, device_id_type=MESH)

        multiply(piece, a_far, b_far, total, c_ref)

    for idx, send in enumerate(a_sends):
        if idx != TURN:
            send.wait_send()

    @pl.when(row == 1)
    def _():
        a_sends[TURN].wait_send()

    for value, b_buf in enumerate((b_near, b_far)):

        @pl.when(slot == value)
        def _():
            for send in sends_of_b(b_buf):
                send.wait_send()


def second_kernel(a_ref, token_ref, b_far, low_ref, c_ref, a_far, total, asend_sem, arecv_sem):
    del token_ref
    layer, _, across, _, _ = place()
    bottom, cols = c_ref.shape
    rows = a_ref.shape[0] // 2

    barrier = pltpu.get_barrier_semaphore()
    pl.semaphore_signal(barrier, inc=1, device_id=across, device_id_type=MESH)
    pl.semaphore_wait(barrier, 1)
    a_sends = sends_of(SECOND, a_ref, layer * rows + rows - bottom, a_far, asend_sem, arecv_sem, across)
    for send in a_sends:
        send.start()
    total[...] = low_ref[...]
    for idx, piece in enumerate(SECOND):
        a_sends[idx].wait_recv()
        multiply(piece, a_far, b_far, total, c_ref)
    for send in a_sends:
        send.wait_send()


def write_top(top_ref, out_ref, token_ref, sem):
    copy = pltpu.make_async_copy(top_ref, out_ref.at[pl.ds(0, top_ref.shape[0]), :], sem)
    copy.start()
    token_ref[...] = jnp.zeros_like(token_ref)
    copy.wait()


def write_bottom(half_ref, low_ref, out_ref, sem):
    del half_ref
    rows, bottom = out_ref.shape[0], low_ref.shape[0]
    copy = pltpu.make_async_copy(low_ref, out_ref.at[pl.ds(rows - bottom, bottom), :], sem)
    copy.start()
    copy.wait()


def solution(mesh):
    depth_n = mesh.shape["depth"]
    dma = pltpu.SemaphoreType.DMA
    hbm, vmem = pl.BlockSpec(memory_space=pltpu.HBM), pl.BlockSpec(memory_space=pltpu.VMEM)

    def local_mm(a_blk, b_blk):
        rows = a_blk.shape[0] // depth_n
        depth, cols = b_blk.shape
        c_type = jax.ShapeDtypeStruct((rows, cols), jnp.bfloat16)
        params = functools.partial(pltpu.CompilerParams, has_side_effects=True)
        c_top, b_far, low = pl.pallas_call(
            first_kernel,
            out_shape=(
                pltpu.VMEM((rows - BOTTOM, cols), jnp.bfloat16),
                pltpu.VMEM((depth, cols), jnp.bfloat16),
                pltpu.VMEM((BOTTOM, cols), jnp.float32),
            ),
            in_specs=[hbm, hbm],
            out_specs=(vmem, vmem, vmem),
            scratch_shapes=[
                pltpu.VMEM((rows, depth), jnp.bfloat16),
                pltpu.VMEM((rows - BOTTOM, depth), jnp.bfloat16),
                pltpu.VMEM((depth, cols), jnp.bfloat16),
                pltpu.VMEM((rows - BOTTOM, cols), jnp.float32),
                dma,
                dma,
                dma((B_PARTS,)),
                dma((B_PARTS,)),
                dma((len(FIRST),)),
                dma((len(FIRST),)),
                pltpu.SemaphoreType.REGULAR,
                pltpu.SemaphoreType.REGULAR,
            ],
            compiler_params=params(collective_id=0, vmem_limit_bytes=40 * 1024 * 1024),
            cost_estimate=pl.CostEstimate(flops=4 * rows * depth * cols, bytes_accessed=12 * depth * cols, transcendentals=0),
        )(a_blk, b_blk)
        written, token = pl.pallas_call(
            write_top,
            out_shape=(c_type, pltpu.VMEM((8, 128), jnp.float32)),
            in_specs=[vmem],
            out_specs=(hbm, vmem),
            scratch_shapes=[dma],
            compiler_params=pltpu.CompilerParams(vmem_limit_bytes=16 * 1024 * 1024),
        )(c_top)
        c_low = pl.pallas_call(
            second_kernel,
            out_shape=pltpu.VMEM((BOTTOM, cols), jnp.bfloat16),
            in_specs=[hbm, vmem, vmem, vmem],
            out_specs=vmem,
            scratch_shapes=[
                pltpu.VMEM((BOTTOM, depth), jnp.bfloat16),
                pltpu.VMEM((BOTTOM, cols), jnp.float32),
                dma((len(SECOND),)),
                dma((len(SECOND),)),
            ],
            compiler_params=params(collective_id=1, vmem_limit_bytes=16 * 1024 * 1024),
        )(a_blk, token, b_far, low)
        return pl.pallas_call(
            write_bottom,
            out_shape=c_type,
            in_specs=[hbm, vmem],
            out_specs=hbm,
            scratch_shapes=[dma],
            input_output_aliases={0: 0},
            compiler_params=pltpu.CompilerParams(vmem_limit_bytes=16 * 1024 * 1024),
        )(written, c_low)

    return jax.shard_map(
        local_mm, mesh=mesh, in_specs=(P("row", "col"), P("row", "col")), out_specs=P(("row", "depth"), "col"), check_vma=False
    )
```

```python
import functools

import jax
import jax.numpy as jnp
from jax import lax
from jax.experimental import pallas as pl
from jax.experimental.pallas import tpu as pltpu
from jax.sharding import PartitionSpec as P

MESH = pl.DeviceIdType.MESH
BOTTOM = 192
FIRST = (
    (0, 256, 0, 2048),
    (256, 256, 0, 2048),
    (632, 8, 0, 2048),
    (512, 120, 0, 2048),
    (640, 64, 0, 2048),
    (704, 128, 0, 512),
    (704, 128, 512, 512),
    (704, 128, 1024, 512),
    (704, 128, 1536, 512),
)
SECOND = (
    (0, 192, 0, 1024),
    (0, 192, 1024, 512),
    (0, 192, 1536, 256),
    (0, 128, 1792, 256),
    (128, 64, 1792, 256),
)
AROUND = 2
HOLD = 4
TURN = 5
B_PARTS = 4
TILE_N = 256


def place():
    layer, col, row = lax.axis_index("depth"), lax.axis_index("col"), lax.axis_index("row")
    return layer, col, row, (layer, 1 - col, row), (layer, col, 1 - row), lax.rem(row + col, 2)


def sends_of(pieces, a_ref, first_row, a_far, send_sem, recv_sem, device):
    return [
        pltpu.make_async_remote_copy(
            src_ref=a_ref.at[pl.ds(first_row + r0, nr), pl.ds(k0, nk)],
            dst_ref=a_far.at[pl.ds(r0, nr), pl.ds(k0, nk)],
            send_sem=send_sem.at[idx],
            recv_sem=recv_sem.at[idx],
            device_id=device,
            device_id_type=MESH,
        )
        for idx, (r0, nr, k0, nk) in enumerate(pieces)
    ]


def multiply(piece, a_far, b_far, total, c_ref):
    r0, nr, k0, nk = piece
    depth, cols = b_far.shape
    r, k = pl.ds(r0, nr), pl.ds(k0, nk)

    def add(c):
        sums = total[r, c] + jnp.dot(a_far[r, k], b_far[k, c], preferred_element_type=jnp.float32)
        if k0 + nk == depth:
            c_ref[r, c] = sums.astype(c_ref.dtype)
        else:
            total[r, c] = sums

    if nk <= 512:
        for tile in range(4):
            add(pl.ds(tile * (cols // 4), cols // 4))
    else:

        @pl.loop(0, cols // TILE_N)
        def _(tile):
            add(pl.ds(pl.multiple_of(tile * TILE_N, TILE_N), TILE_N))


def first_kernel(
    a_ref,
    b_ref,
    c_ref,
    b_far,
    low,
    a_own,
    a_far,
    b_near,
    total,
    own_sem,
    bown_sem,
    bsend_sem,
    brecv_sem,
    asend_sem,
    arecv_sem,
    ready_sem,
    turn_sem,
    passing,
    pass_sem,
):
    layer, col, row, across, beside, slot = place()
    top, cols = c_ref.shape
    rows, depth = a_own.shape
    base = layer * rows

    barrier = pltpu.get_barrier_semaphore()
    pl.semaphore_signal(barrier, inc=1, device_id=across, device_id_type=MESH)

    upper = jnp.logical_and(row == 1, layer == 0)
    lower = jnp.logical_and(row == 1, layer == 1)
    below = (1 - layer, col, row)

    @pl.when(row == 1)
    def _():
        pl.semaphore_signal(barrier, inc=1, device_id=beside, device_id_type=MESH)

    @pl.when(upper)
    def _():
        pl.semaphore_signal(barrier, inc=1, device_id=below, device_id_type=MESH)

    @pl.when(lower)
    def _():
        pl.semaphore_wait(barrier, 2)

    @pl.when(upper)
    def _():
        pl.semaphore_wait(barrier, 1)

    @pl.when(row == 0)
    def _():
        pl.semaphore_wait(barrier, 2)
        pl.semaphore_signal(ready_sem, inc=1, device_id=beside, device_id_type=MESH)

    a_sends = sends_of(FIRST, a_ref, base, a_far, asend_sem, arecv_sem, across)
    r0, nr, k0, nk = FIRST[AROUND]
    to_relay = pltpu.make_async_remote_copy(
        src_ref=a_ref.at[pl.ds(r0, nr), pl.ds(k0, nk)],
        dst_ref=passing,
        send_sem=pass_sem.at[0],
        recv_sem=pass_sem.at[1],
        device_id=across,
        device_id_type=MESH,
    )
    from_relay = pltpu.make_async_remote_copy(
        src_ref=passing,
        dst_ref=a_far.at[pl.ds(r0, nr), pl.ds(k0, nk)],
        send_sem=pass_sem.at[2],
        recv_sem=arecv_sem.at[AROUND],
        device_id=below,
        device_id_type=MESH,
    )
    part = depth // B_PARTS

    def sends_of_b(b_buf):
        return [
            pltpu.make_async_remote_copy(
                src_ref=b_ref.at[pl.ds(idx * part, part), :],
                dst_ref=b_buf.at[pl.ds(idx * part, part), :],
                send_sem=bsend_sem.at[idx],
                recv_sem=brecv_sem.at[idx],
                device_id=beside,
                device_id_type=MESH,
            )
            for idx in range(B_PARTS)
        ]

    def own_of_b(b_buf):
        return pltpu.make_async_copy(b_ref, b_buf, bown_sem)

    own_a = pltpu.make_async_copy(a_ref.at[pl.ds(base, rows), :], a_own, own_sem)

    a_sends[0].start()

    @pl.when(row == 1)
    def _():
        pl.semaphore_wait(ready_sem, 1)

    for value, b_buf in enumerate((b_near, b_far)):

        @pl.when(slot == value)
        def _():
            for send in sends_of_b(b_buf):
                send.start()

    @pl.when(lower)
    def _():
        to_relay.start()

    a_sends[1].start()

    @pl.when(jnp.logical_not(upper))
    def _():
        a_sends[AROUND].start()

    for send in a_sends[AROUND + 1 : HOLD]:
        send.start()

    @pl.when(row == 0)
    def _():
        for send in a_sends[HOLD:]:
            send.start()

    own_a.start()
    for value, b_buf in enumerate((b_near, b_far)):

        @pl.when(slot == value)
        def _():
            own_of_b(b_buf).start()

    own_a.wait()
    for value, (b_mine, b_other) in enumerate(((b_near, b_far), (b_far, b_near))):

        @pl.when(slot == value)
        def _():
            own_of_b(b_mine).wait()
            for send in sends_of_b(b_other):
                send.wait_recv()

    col_tiles = cols // TILE_N
    tile_m = top // 4

    @pl.loop(0, 4 * col_tiles)
    def _(tile):
        r = pl.ds(pl.multiple_of((tile // col_tiles) * tile_m, 16), tile_m)
        c = pl.ds(pl.multiple_of((tile % col_tiles) * TILE_N, TILE_N), TILE_N)
        total[r, c] = jnp.dot(a_own[r, :], b_near[:, c], preferred_element_type=jnp.float32)

    @pl.loop(0, col_tiles)
    def _(tile):
        c = pl.ds(pl.multiple_of(tile * TILE_N, TILE_N), TILE_N)
        low[:, c] = jnp.dot(a_own[pl.ds(top, rows - top), :], b_near[:, c], preferred_element_type=jnp.float32)

    for idx, piece in enumerate(FIRST):
        if idx == HOLD:

            @pl.when(row == 1)
            def _():
                pl.semaphore_wait(turn_sem, 1)
                for send in a_sends[HOLD:]:
                    send.start()

        a_sends[idx].wait_recv()
        if idx == TURN:

            @pl.when(row == 0)
            def _():
                a_sends[TURN].wait_send()
                pl.semaphore_signal(turn_sem, inc=1, device_id=beside, device_id_type=MESH)

        if idx == AROUND + 1:
            piece = (piece[0], piece[1] + FIRST[AROUND][1], *piece[2:])
        if idx != AROUND:
            multiply(piece, a_far, b_far, total, c_ref)
        if idx == 0:

            @pl.when(lower)
            def _():
                to_relay.wait_recv()
                from_relay.start()

    for idx, send in enumerate(a_sends):
        if idx not in (TURN, AROUND):
            send.wait_send()

    @pl.when(jnp.logical_not(upper))
    def _():
        a_sends[AROUND].wait_send()

    @pl.when(lower)
    def _():
        to_relay.wait_send()
        from_relay.wait_send()

    @pl.when(row == 1)
    def _():
        a_sends[TURN].wait_send()

    for value, b_buf in enumerate((b_near, b_far)):

        @pl.when(slot == value)
        def _():
            for send in sends_of_b(b_buf):
                send.wait_send()


def second_kernel(a_ref, token_ref, b_far, low_ref, c_ref, a_far, total, asend_sem, arecv_sem):
    del token_ref
    layer, _, _, across, _, _ = place()
    bottom, rows = total.shape[0], a_ref.shape[0] // 2

    barrier = pltpu.get_barrier_semaphore()
    pl.semaphore_signal(barrier, inc=1, device_id=across, device_id_type=MESH)
    pl.semaphore_wait(barrier, 1)
    a_sends = sends_of(SECOND, a_ref, layer * rows + rows - bottom, a_far, asend_sem, arecv_sem, across)
    for send in a_sends:
        send.start()
    total[...] = low_ref[...]
    for idx, piece in enumerate(SECOND):
        a_sends[idx].wait_recv()
        if idx + 1 < len(SECOND):
            multiply(piece, a_far, b_far, total, c_ref)
    for send in a_sends:
        send.wait_send()


def write_top(top_ref, out_ref, token_ref, sem):
    copy = pltpu.make_async_copy(top_ref, out_ref.at[pl.ds(0, top_ref.shape[0]), :], sem)
    copy.start()
    token_ref[...] = jnp.zeros_like(token_ref)
    copy.wait()


def write_bottom(half_ref, ready_ref, a_far, total, b_far, out_ref, last, ready_sem, last_sem):
    del half_ref
    rows, ready = out_ref.shape[0], ready_ref.shape[0]
    r0, nr, k0, nk = SECOND[-1]
    first_row = rows - r0 - nr
    ready_copy = pltpu.make_async_copy(ready_ref, out_ref.at[pl.ds(first_row, ready), :], ready_sem)
    ready_copy.start()
    tn = last.shape[1] // 4
    for tile in range(4):
        r, k, c = pl.ds(r0, nr), pl.ds(k0, nk), pl.ds(tile * tn, tn)
        sums = total[r, c] + jnp.dot(a_far[r, k], b_far[k, c], preferred_element_type=jnp.float32)
        last[:, c] = sums.astype(last.dtype)
    last_copy = pltpu.make_async_copy(last, out_ref.at[pl.ds(first_row + r0, nr), :], last_sem)
    last_copy.start()
    ready_copy.wait()
    last_copy.wait()


def solution(mesh):
    depth_n = mesh.shape["depth"]
    dma = pltpu.SemaphoreType.DMA
    hbm, vmem = pl.BlockSpec(memory_space=pltpu.HBM), pl.BlockSpec(memory_space=pltpu.VMEM)

    def local_mm(a_blk, b_blk):
        rows = a_blk.shape[0] // depth_n
        depth, cols = b_blk.shape
        c_type = jax.ShapeDtypeStruct((rows, cols), jnp.bfloat16)
        params = functools.partial(pltpu.CompilerParams, has_side_effects=True)
        c_top, b_far, low = pl.pallas_call(
            first_kernel,
            out_shape=(
                pltpu.VMEM((rows - BOTTOM, cols), jnp.bfloat16),
                pltpu.VMEM((depth, cols), jnp.bfloat16),
                pltpu.VMEM((BOTTOM, cols), jnp.float32),
            ),
            in_specs=[hbm, hbm],
            out_specs=(vmem, vmem, vmem),
            scratch_shapes=[
                pltpu.VMEM((rows, depth), jnp.bfloat16),
                pltpu.VMEM((rows - BOTTOM, depth), jnp.bfloat16),
                pltpu.VMEM((depth, cols), jnp.bfloat16),
                pltpu.VMEM((rows - BOTTOM, cols), jnp.float32),
                dma,
                dma,
                dma((B_PARTS,)),
                dma((B_PARTS,)),
                dma((len(FIRST),)),
                dma((len(FIRST),)),
                pltpu.SemaphoreType.REGULAR,
                pltpu.SemaphoreType.REGULAR,
                pltpu.VMEM(FIRST[AROUND][1::2], jnp.bfloat16),
                dma((3,)),
            ],
            compiler_params=params(collective_id=0, vmem_limit_bytes=40 * 1024 * 1024),
            cost_estimate=pl.CostEstimate(flops=4 * rows * depth * cols, bytes_accessed=12 * depth * cols, transcendentals=0),
        )(a_blk, b_blk)
        written, token = pl.pallas_call(
            write_top,
            out_shape=(c_type, pltpu.VMEM((8, 128), jnp.float32)),
            in_specs=[vmem],
            out_specs=(hbm, vmem),
            scratch_shapes=[dma],
            compiler_params=pltpu.CompilerParams(vmem_limit_bytes=16 * 1024 * 1024),
        )(c_top)
        c_ready, a_far, low_total = pl.pallas_call(
            second_kernel,
            out_shape=(
                pltpu.VMEM((SECOND[-1][0], cols), jnp.bfloat16),
                pltpu.VMEM((BOTTOM, depth), jnp.bfloat16),
                pltpu.VMEM((BOTTOM, cols), jnp.float32),
            ),
            in_specs=[hbm, vmem, vmem, vmem],
            out_specs=(vmem, vmem, vmem),
            scratch_shapes=[
                dma((len(SECOND),)),
                dma((len(SECOND),)),
            ],
            compiler_params=params(collective_id=1, vmem_limit_bytes=16 * 1024 * 1024),
        )(a_blk, token, b_far, low)
        return pl.pallas_call(
            write_bottom,
            out_shape=c_type,
            in_specs=[hbm, vmem, vmem, vmem, vmem],
            out_specs=hbm,
            scratch_shapes=[pltpu.VMEM((SECOND[-1][1], cols), jnp.bfloat16), dma, dma],
            input_output_aliases={0: 0},
            compiler_params=pltpu.CompilerParams(vmem_limit_bytes=16 * 1024 * 1024),
        )(written, c_ready, a_far, low_total, b_far)

    return jax.shard_map(
        local_mm, mesh=mesh, in_specs=(P("row", "col"), P("row", "col")), out_specs=P(("row", "depth"), "col"), check_vma=False
    )
```

```python
import functools

import jax
import jax.numpy as jnp
from jax import lax
from jax.experimental import pallas as pl
from jax.experimental.pallas import tpu as pltpu
from jax.sharding import PartitionSpec as P

MESH = pl.DeviceIdType.MESH
BOTTOM = 192
FIRST = (
    (0, 256, 0, 2048),
    (256, 256, 0, 2048),
    (632, 8, 0, 2048),
    (512, 120, 0, 2048),
    (640, 64, 0, 2048),
    (704, 128, 0, 512),
    (704, 128, 512, 512),
    (704, 128, 1024, 512),
    (704, 128, 1536, 512),
)
SECOND = (
    (0, 192, 0, 1024),
    (0, 192, 1024, 512),
    (0, 192, 1536, 256),
    (0, 128, 1792, 256),
    (128, 64, 1792, 256),
)
AROUND = 2
HOLD = 4
TURN = 5
B_PARTS = 4
TILE_N = 256


def place():
    layer, col, row = lax.axis_index("depth"), lax.axis_index("col"), lax.axis_index("row")
    return layer, col, row, (layer, 1 - col, row), (layer, col, 1 - row), lax.rem(row + col, 2)


def sends_of(pieces, a_src, a_far, send_sem, recv_sem, device):
    return [
        pltpu.make_async_remote_copy(
            src_ref=a_src.at[pl.ds(r0, nr), pl.ds(k0, nk)],
            dst_ref=a_far.at[pl.ds(r0, nr), pl.ds(k0, nk)],
            send_sem=send_sem.at[idx],
            recv_sem=recv_sem.at[idx],
            device_id=device,
            device_id_type=MESH,
        )
        for idx, (r0, nr, k0, nk) in enumerate(pieces)
    ]


def multiply(piece, a_far, b_far, total, c_ref):
    r0, nr, k0, nk = piece
    depth, cols = b_far.shape
    r, k = pl.ds(r0, nr), pl.ds(k0, nk)

    def add(c):
        sums = total[r, c] + jnp.dot(a_far[r, k], b_far[k, c], preferred_element_type=jnp.float32)
        if k0 + nk == depth:
            c_ref[r, c] = sums.astype(c_ref.dtype)
        else:
            total[r, c] = sums

    if nk <= 512:
        for tile in range(4):
            add(pl.ds(tile * (cols // 4), cols // 4))
    else:

        @pl.loop(0, cols // TILE_N)
        def _(tile):
            add(pl.ds(pl.multiple_of(tile * TILE_N, TILE_N), TILE_N))


def first_kernel(
    a_ref,
    b_ref,
    c_ref,
    b_far,
    low,
    a_low,
    a_own,
    a_far,
    b_near,
    total,
    own_sem,
    low_sem,
    bown_sem,
    bsend_sem,
    brecv_sem,
    asend_sem,
    arecv_sem,
    ready_sem,
    turn_sem,
    passing,
    pass_sem,
):
    layer, col, row, across, beside, slot = place()
    top, cols = c_ref.shape
    bottom, depth = a_low.shape
    base = layer * (top + bottom)

    barrier = pltpu.get_barrier_semaphore()
    pl.semaphore_signal(barrier, inc=1, device_id=across, device_id_type=MESH)

    upper = jnp.logical_and(row == 1, layer == 0)
    lower = jnp.logical_and(row == 1, layer == 1)
    below = (1 - layer, col, row)

    @pl.when(row == 1)
    def _():
        pl.semaphore_signal(barrier, inc=1, device_id=beside, device_id_type=MESH)

    @pl.when(upper)
    def _():
        pl.semaphore_signal(barrier, inc=1, device_id=below, device_id_type=MESH)

    @pl.when(lower)
    def _():
        pl.semaphore_wait(barrier, 2)

    @pl.when(upper)
    def _():
        pl.semaphore_wait(barrier, 1)

    @pl.when(row == 0)
    def _():
        pl.semaphore_wait(barrier, 2)
        pl.semaphore_signal(ready_sem, inc=1, device_id=beside, device_id_type=MESH)

    a_sends = sends_of(FIRST, a_own, a_far, asend_sem, arecv_sem, across)
    first_rows = a_ref.at[pl.ds(base, FIRST[0][1]), :]
    a_sends[0] = sends_of(FIRST[:1], first_rows, a_far, asend_sem, arecv_sem, across)[0]
    r0, nr, k0, nk = FIRST[AROUND]
    to_relay = pltpu.make_async_remote_copy(
        src_ref=a_ref.at[pl.ds(r0, nr), pl.ds(k0, nk)],
        dst_ref=passing,
        send_sem=pass_sem.at[0],
        recv_sem=pass_sem.at[1],
        device_id=across,
        device_id_type=MESH,
    )
    from_relay = pltpu.make_async_remote_copy(
        src_ref=passing,
        dst_ref=a_far.at[pl.ds(r0, nr), pl.ds(k0, nk)],
        send_sem=pass_sem.at[2],
        recv_sem=arecv_sem.at[AROUND],
        device_id=below,
        device_id_type=MESH,
    )
    part = depth // B_PARTS

    def sends_of_b(b_buf):
        return [
            pltpu.make_async_remote_copy(
                src_ref=b_ref.at[pl.ds(idx * part, part), :],
                dst_ref=b_buf.at[pl.ds(idx * part, part), :],
                send_sem=bsend_sem.at[idx],
                recv_sem=brecv_sem.at[idx],
                device_id=beside,
                device_id_type=MESH,
            )
            for idx in range(B_PARTS)
        ]

    def own_of_b(b_buf):
        return pltpu.make_async_copy(b_ref, b_buf, bown_sem)

    own_a = pltpu.make_async_copy(a_ref.at[pl.ds(base, top), :], a_own, own_sem)
    own_low = pltpu.make_async_copy(a_ref.at[pl.ds(base + top, bottom), :], a_low, low_sem)

    a_sends[0].start()
    own_a.start()
    own_low.start()

    @pl.when(row == 1)
    def _():
        pl.semaphore_wait(ready_sem, 1)

    for value, b_buf in enumerate((b_near, b_far)):

        @pl.when(slot == value)
        def _():
            for send in sends_of_b(b_buf):
                send.start()

    @pl.when(lower)
    def _():
        to_relay.start()

    own_a.wait()
    a_sends[1].start()

    @pl.when(jnp.logical_not(upper))
    def _():
        a_sends[AROUND].start()

    for send in a_sends[AROUND + 1 : HOLD]:
        send.start()

    @pl.when(row == 0)
    def _():
        for send in a_sends[HOLD:]:
            send.start()

    for value, b_buf in enumerate((b_near, b_far)):

        @pl.when(slot == value)
        def _():
            own_of_b(b_buf).start()

    own_low.wait()
    for value, (b_mine, b_other) in enumerate(((b_near, b_far), (b_far, b_near))):

        @pl.when(slot == value)
        def _():
            own_of_b(b_mine).wait()
            for send in sends_of_b(b_other):
                send.wait_recv()

    col_tiles = cols // TILE_N
    tile_m = top // 4

    @pl.loop(0, 4 * col_tiles)
    def _(tile):
        r = pl.ds(pl.multiple_of((tile // col_tiles) * tile_m, 16), tile_m)
        c = pl.ds(pl.multiple_of((tile % col_tiles) * TILE_N, TILE_N), TILE_N)
        total[r, c] = jnp.dot(a_own[r, :], b_near[:, c], preferred_element_type=jnp.float32)

    @pl.loop(0, col_tiles)
    def _(tile):
        c = pl.ds(pl.multiple_of(tile * TILE_N, TILE_N), TILE_N)
        low[:, c] = jnp.dot(a_low[...], b_near[:, c], preferred_element_type=jnp.float32)

    for idx, piece in enumerate(FIRST):
        if idx == HOLD:

            @pl.when(row == 1)
            def _():
                pl.semaphore_wait(turn_sem, 1)
                for send in a_sends[HOLD:]:
                    send.start()

        a_sends[idx].wait_recv()
        if idx == TURN:

            @pl.when(row == 0)
            def _():
                a_sends[TURN].wait_send()
                pl.semaphore_signal(turn_sem, inc=1, device_id=beside, device_id_type=MESH)

        if idx == AROUND + 1:
            piece = (piece[0], piece[1] + FIRST[AROUND][1], *piece[2:])
        if idx != AROUND:
            multiply(piece, a_far, b_far, total, c_ref)
        if idx == 0:

            @pl.when(lower)
            def _():
                to_relay.wait_recv()
                from_relay.start()

    for idx, send in enumerate(a_sends):
        if idx not in (TURN, AROUND):
            send.wait_send()

    @pl.when(jnp.logical_not(upper))
    def _():
        a_sends[AROUND].wait_send()

    @pl.when(lower)
    def _():
        to_relay.wait_send()
        from_relay.wait_send()

    @pl.when(row == 1)
    def _():
        a_sends[TURN].wait_send()

    for value, b_buf in enumerate((b_near, b_far)):

        @pl.when(slot == value)
        def _():
            for send in sends_of_b(b_buf):
                send.wait_send()


def second_kernel(a_low, token_ref, b_far, low_ref, c_ref, a_far, total, asend_sem, arecv_sem):
    del token_ref
    _, _, _, across, _, _ = place()

    barrier = pltpu.get_barrier_semaphore()
    pl.semaphore_signal(barrier, inc=1, device_id=across, device_id_type=MESH)
    pl.semaphore_wait(barrier, 1)
    a_sends = sends_of(SECOND, a_low, a_far, asend_sem, arecv_sem, across)
    for send in a_sends:
        send.start()
    total[...] = low_ref[...]
    for idx, piece in enumerate(SECOND):
        a_sends[idx].wait_recv()
        if idx + 1 < len(SECOND):
            multiply(piece, a_far, b_far, total, c_ref)
    for send in a_sends:
        send.wait_send()


def write_top(top_ref, out_ref, token_ref, sem):
    copy = pltpu.make_async_copy(top_ref, out_ref.at[pl.ds(0, top_ref.shape[0]), :], sem)
    copy.start()
    token_ref[...] = jnp.zeros_like(token_ref)
    copy.wait()


def write_bottom(half_ref, ready_ref, a_far, total, b_far, out_ref, last, ready_sem, last_sem):
    del half_ref
    rows, ready = out_ref.shape[0], ready_ref.shape[0]
    r0, nr, k0, nk = SECOND[-1]
    first_row = rows - r0 - nr
    ready_copy = pltpu.make_async_copy(ready_ref, out_ref.at[pl.ds(first_row, ready), :], ready_sem)
    ready_copy.start()
    tn = last.shape[1] // 4
    copies = [ready_copy]
    for tile in range(4):
        r, k, c = pl.ds(r0, nr), pl.ds(k0, nk), pl.ds(tile * tn, tn)
        sums = total[r, c] + jnp.dot(a_far[r, k], b_far[k, c], preferred_element_type=jnp.float32)
        last[:, c] = sums.astype(last.dtype)
        copies.append(pltpu.make_async_copy(last.at[:, c], out_ref.at[pl.ds(first_row + r0, nr), c], last_sem.at[tile]))
        copies[-1].start()
    for copy in copies:
        copy.wait()


def solution(mesh):
    depth_n = mesh.shape["depth"]
    dma = pltpu.SemaphoreType.DMA
    hbm, vmem = pl.BlockSpec(memory_space=pltpu.HBM), pl.BlockSpec(memory_space=pltpu.VMEM)

    def local_mm(a_blk, b_blk):
        rows = a_blk.shape[0] // depth_n
        depth, cols = b_blk.shape
        c_type = jax.ShapeDtypeStruct((rows, cols), jnp.bfloat16)
        params = functools.partial(pltpu.CompilerParams, has_side_effects=True)
        c_top, b_far, low, a_low = pl.pallas_call(
            first_kernel,
            out_shape=(
                pltpu.VMEM((rows - BOTTOM, cols), jnp.bfloat16),
                pltpu.VMEM((depth, cols), jnp.bfloat16),
                pltpu.VMEM((BOTTOM, cols), jnp.float32),
                pltpu.VMEM((BOTTOM, depth), jnp.bfloat16),
            ),
            in_specs=[hbm, hbm],
            out_specs=(vmem, vmem, vmem, vmem),
            scratch_shapes=[
                pltpu.VMEM((rows - BOTTOM, depth), jnp.bfloat16),
                pltpu.VMEM((rows - BOTTOM, depth), jnp.bfloat16),
                pltpu.VMEM((depth, cols), jnp.bfloat16),
                pltpu.VMEM((rows - BOTTOM, cols), jnp.float32),
                dma,
                dma,
                dma,
                dma((B_PARTS,)),
                dma((B_PARTS,)),
                dma((len(FIRST),)),
                dma((len(FIRST),)),
                pltpu.SemaphoreType.REGULAR,
                pltpu.SemaphoreType.REGULAR,
                pltpu.VMEM(FIRST[AROUND][1::2], jnp.bfloat16),
                dma((3,)),
            ],
            compiler_params=params(collective_id=0, vmem_limit_bytes=40 * 1024 * 1024),
            cost_estimate=pl.CostEstimate(flops=4 * rows * depth * cols, bytes_accessed=12 * depth * cols, transcendentals=0),
        )(a_blk, b_blk)
        written, token = pl.pallas_call(
            write_top,
            out_shape=(c_type, pltpu.VMEM((8, 128), jnp.float32)),
            in_specs=[vmem],
            out_specs=(hbm, vmem),
            scratch_shapes=[dma],
            compiler_params=pltpu.CompilerParams(vmem_limit_bytes=16 * 1024 * 1024),
        )(c_top)
        c_ready, a_far, low_total = pl.pallas_call(
            second_kernel,
            out_shape=(
                pltpu.VMEM((SECOND[-1][0], cols), jnp.bfloat16),
                pltpu.VMEM((BOTTOM, depth), jnp.bfloat16),
                pltpu.VMEM((BOTTOM, cols), jnp.float32),
            ),
            in_specs=[vmem, vmem, vmem, vmem],
            out_specs=(vmem, vmem, vmem),
            scratch_shapes=[
                dma((len(SECOND),)),
                dma((len(SECOND),)),
            ],
            compiler_params=params(collective_id=1, vmem_limit_bytes=16 * 1024 * 1024),
        )(a_low, token, b_far, low)
        return pl.pallas_call(
            write_bottom,
            out_shape=c_type,
            in_specs=[hbm, vmem, vmem, vmem, vmem],
            out_specs=hbm,
            scratch_shapes=[pltpu.VMEM((SECOND[-1][1], cols), jnp.bfloat16), dma, dma((4,))],
            input_output_aliases={0: 0},
            compiler_params=pltpu.CompilerParams(vmem_limit_bytes=16 * 1024 * 1024),
        )(written, c_ready, a_far, low_total, b_far)

    return jax.shard_map(
        local_mm, mesh=mesh, in_specs=(P("row", "col"), P("row", "col")), out_specs=P(("row", "depth"), "col"), check_vma=False
    )
```

```python
import functools

import jax
import jax.numpy as jnp
from jax import lax
from jax.experimental import pallas as pl
from jax.experimental.pallas import tpu as pltpu
from jax.sharding import PartitionSpec as P

MESH = pl.DeviceIdType.MESH
BOTTOM = 192
FIRST = (
    (0, 256, 0, 2048),
    (256, 256, 0, 2048),
    (632, 8, 0, 2048),
    (512, 120, 0, 2048),
    (640, 64, 0, 2048),
    (704, 128, 0, 512),
    (704, 128, 512, 512),
    (704, 128, 1024, 512),
    (704, 128, 1536, 512),
)
SECOND = (
    (0, 192, 0, 1024),
    (0, 192, 1024, 512),
    (0, 192, 1536, 256),
    (0, 128, 1792, 256),
    (128, 64, 1792, 256),
)
AROUND = 2
HOLD = 4
TURN = 5
B_PARTS = 4
TILE_N = 256


def place():
    layer, col, row = lax.axis_index("depth"), lax.axis_index("col"), lax.axis_index("row")
    return layer, col, row, (layer, 1 - col, row), (layer, col, 1 - row), lax.rem(row + col, 2)


def sends_of(pieces, a_src, a_far, send_sem, recv_sem, device):
    return [
        pltpu.make_async_remote_copy(
            src_ref=a_src.at[pl.ds(r0, nr), pl.ds(k0, nk)],
            dst_ref=a_far.at[pl.ds(r0, nr), pl.ds(k0, nk)],
            send_sem=send_sem.at[idx],
            recv_sem=recv_sem.at[idx],
            device_id=device,
            device_id_type=MESH,
        )
        for idx, (r0, nr, k0, nk) in enumerate(pieces)
    ]


def multiply(piece, a_far, b_far, total, c_ref):
    r0, nr, k0, nk = piece
    depth, cols = b_far.shape
    r, k = pl.ds(r0, nr), pl.ds(k0, nk)

    def add(c):
        sums = total[r, c] + jnp.dot(a_far[r, k], b_far[k, c], preferred_element_type=jnp.float32)
        if k0 + nk == depth:
            c_ref[r, c] = sums.astype(c_ref.dtype)
        else:
            total[r, c] = sums

    if nk <= 512:
        for tile in range(4):
            add(pl.ds(tile * (cols // 4), cols // 4))
    else:

        @pl.loop(0, cols // TILE_N)
        def _(tile):
            add(pl.ds(pl.multiple_of(tile * TILE_N, TILE_N), TILE_N))


def first_kernel(
    a_ref,
    b_ref,
    c_ref,
    b_far,
    low,
    a_low,
    a_own,
    a_far,
    b_near,
    total,
    own_sem,
    low_sem,
    bown_sem,
    bsend_sem,
    brecv_sem,
    asend_sem,
    arecv_sem,
    ready_sem,
    turn_sem,
    passing,
    pass_sem,
):
    layer, col, row, across, beside, slot = place()
    top, cols = c_ref.shape
    bottom, depth = a_low.shape
    base = layer * (top + bottom)

    barrier = pltpu.get_barrier_semaphore()
    pl.semaphore_signal(barrier, inc=1, device_id=across, device_id_type=MESH)

    upper = jnp.logical_and(row == 1, layer == 0)
    lower = jnp.logical_and(row == 1, layer == 1)
    below = (1 - layer, col, row)

    @pl.when(row == 1)
    def _():
        pl.semaphore_signal(barrier, inc=1, device_id=beside, device_id_type=MESH)

    @pl.when(upper)
    def _():
        pl.semaphore_signal(barrier, inc=1, device_id=below, device_id_type=MESH)

    @pl.when(lower)
    def _():
        pl.semaphore_wait(barrier, 2)

    @pl.when(upper)
    def _():
        pl.semaphore_wait(barrier, 1)

    @pl.when(row == 0)
    def _():
        pl.semaphore_wait(barrier, 2)
        pl.semaphore_signal(ready_sem, inc=1, device_id=beside, device_id_type=MESH)

    a_sends = sends_of(FIRST, a_own, a_far, asend_sem, arecv_sem, across)
    first_rows = a_ref.at[pl.ds(base, FIRST[0][1]), :]
    a_sends[0] = sends_of(FIRST[:1], first_rows, a_far, asend_sem, arecv_sem, across)[0]
    r0, nr, k0, nk = FIRST[AROUND]
    to_relay = pltpu.make_async_remote_copy(
        src_ref=a_ref.at[pl.ds(r0, nr), pl.ds(k0, nk)],
        dst_ref=passing,
        send_sem=pass_sem.at[0],
        recv_sem=pass_sem.at[1],
        device_id=across,
        device_id_type=MESH,
    )
    from_relay = pltpu.make_async_remote_copy(
        src_ref=passing,
        dst_ref=a_far.at[pl.ds(r0, nr), pl.ds(k0, nk)],
        send_sem=pass_sem.at[2],
        recv_sem=arecv_sem.at[AROUND],
        device_id=below,
        device_id_type=MESH,
    )
    part = depth // B_PARTS

    def sends_of_b(b_buf):
        return [
            pltpu.make_async_remote_copy(
                src_ref=b_ref.at[pl.ds(idx * part, part), :],
                dst_ref=b_buf.at[pl.ds(idx * part, part), :],
                send_sem=bsend_sem.at[idx],
                recv_sem=brecv_sem.at[idx],
                device_id=beside,
                device_id_type=MESH,
            )
            for idx in range(B_PARTS)
        ]

    def own_of_b(b_buf):
        return pltpu.make_async_copy(b_ref, b_buf, bown_sem)

    own_a = pltpu.make_async_copy(a_ref.at[pl.ds(base, top), :], a_own, own_sem)
    own_low = pltpu.make_async_copy(a_ref.at[pl.ds(base + top, bottom), :], a_low, low_sem)

    a_sends[0].start()
    own_a.start()
    own_low.start()
    for value, b_buf in enumerate((b_near, b_far)):

        @pl.when(slot == value)
        def _():
            own_of_b(b_buf).start()

    @pl.when(row == 1)
    def _():
        pl.semaphore_wait(ready_sem, 1)

    for value, b_buf in enumerate((b_near, b_far)):

        @pl.when(slot == value)
        def _():
            for send in sends_of_b(b_buf):
                send.start()

    @pl.when(lower)
    def _():
        to_relay.start()

    for value, (b_mine, b_other) in enumerate(((b_near, b_far), (b_far, b_near))):

        @pl.when(slot == value)
        def _():
            for send in sends_of_b(b_other):
                send.wait_recv()
            own_of_b(b_mine).wait()

    own_a.wait()
    own_low.wait()
    a_sends[1].start()

    @pl.when(jnp.logical_not(upper))
    def _():
        a_sends[AROUND].start()

    for send in a_sends[AROUND + 1 : HOLD]:
        send.start()

    @pl.when(row == 0)
    def _():
        for send in a_sends[HOLD:]:
            send.start()

    col_tiles = cols // TILE_N
    tile_m = top // 4

    @pl.loop(0, 4 * col_tiles)
    def _(tile):
        r = pl.ds(pl.multiple_of((tile // col_tiles) * tile_m, 16), tile_m)
        c = pl.ds(pl.multiple_of((tile % col_tiles) * TILE_N, TILE_N), TILE_N)
        total[r, c] = jnp.dot(a_own[r, :], b_near[:, c], preferred_element_type=jnp.float32)

    @pl.loop(0, col_tiles)
    def _(tile):
        c = pl.ds(pl.multiple_of(tile * TILE_N, TILE_N), TILE_N)
        low[:, c] = jnp.dot(a_low[...], b_near[:, c], preferred_element_type=jnp.float32)

    for idx, piece in enumerate(FIRST):
        if idx == HOLD:

            @pl.when(row == 1)
            def _():
                pl.semaphore_wait(turn_sem, 1)
                for send in a_sends[HOLD:]:
                    send.start()

        a_sends[idx].wait_recv()
        if idx == TURN:

            @pl.when(row == 0)
            def _():
                a_sends[TURN].wait_send()
                pl.semaphore_signal(turn_sem, inc=1, device_id=beside, device_id_type=MESH)

        if idx == AROUND + 1:
            piece = (piece[0], piece[1] + FIRST[AROUND][1], *piece[2:])
        if idx != AROUND:
            multiply(piece, a_far, b_far, total, c_ref)
        if idx == 0:

            @pl.when(lower)
            def _():
                to_relay.wait_recv()
                from_relay.start()

    for idx, send in enumerate(a_sends):
        if idx not in (TURN, AROUND):
            send.wait_send()

    @pl.when(jnp.logical_not(upper))
    def _():
        a_sends[AROUND].wait_send()

    @pl.when(lower)
    def _():
        to_relay.wait_send()
        from_relay.wait_send()

    @pl.when(row == 1)
    def _():
        a_sends[TURN].wait_send()

    for value, b_buf in enumerate((b_near, b_far)):

        @pl.when(slot == value)
        def _():
            for send in sends_of_b(b_buf):
                send.wait_send()


def second_kernel(a_low, token_ref, b_far, low_ref, c_ref, a_far, total, asend_sem, arecv_sem):
    del token_ref
    _, _, _, across, _, _ = place()

    barrier = pltpu.get_barrier_semaphore()
    pl.semaphore_signal(barrier, inc=1, device_id=across, device_id_type=MESH)
    pl.semaphore_wait(barrier, 1)
    a_sends = sends_of(SECOND, a_low, a_far, asend_sem, arecv_sem, across)
    for send in a_sends:
        send.start()
    total[...] = low_ref[...]
    for idx, piece in enumerate(SECOND):
        a_sends[idx].wait_recv()
        if idx + 1 < len(SECOND):
            multiply(piece, a_far, b_far, total, c_ref)
    for send in a_sends:
        send.wait_send()


def write_top(top_ref, out_ref, token_ref, sem):
    copy = pltpu.make_async_copy(top_ref, out_ref.at[pl.ds(0, top_ref.shape[0]), :], sem)
    copy.start()
    token_ref[...] = jnp.zeros_like(token_ref)
    copy.wait()


def write_bottom(half_ref, ready_ref, a_far, total, b_far, out_ref, last, ready_sem, last_sem):
    del half_ref
    rows, ready = out_ref.shape[0], ready_ref.shape[0]
    r0, nr, k0, nk = SECOND[-1]
    first_row = rows - r0 - nr
    ready_copy = pltpu.make_async_copy(ready_ref, out_ref.at[pl.ds(first_row, ready), :], ready_sem)
    ready_copy.start()
    tn = last.shape[1] // 4
    copies = [ready_copy]
    for tile in range(4):
        r, k, c = pl.ds(r0, nr), pl.ds(k0, nk), pl.ds(tile * tn, tn)
        sums = total[r, c] + jnp.dot(a_far[r, k], b_far[k, c], preferred_element_type=jnp.float32)
        last[:, c] = sums.astype(last.dtype)
        copies.append(pltpu.make_async_copy(last.at[:, c], out_ref.at[pl.ds(first_row + r0, nr), c], last_sem.at[tile]))
        copies[-1].start()
    for copy in copies:
        copy.wait()


def solution(mesh):
    depth_n = mesh.shape["depth"]
    dma = pltpu.SemaphoreType.DMA
    hbm, vmem = pl.BlockSpec(memory_space=pltpu.HBM), pl.BlockSpec(memory_space=pltpu.VMEM)

    def local_mm(a_blk, b_blk):
        rows = a_blk.shape[0] // depth_n
        depth, cols = b_blk.shape
        c_type = jax.ShapeDtypeStruct((rows, cols), jnp.bfloat16)
        params = functools.partial(pltpu.CompilerParams, has_side_effects=True)
        c_top, b_far, low, a_low = pl.pallas_call(
            first_kernel,
            out_shape=(
                pltpu.VMEM((rows - BOTTOM, cols), jnp.bfloat16),
                pltpu.VMEM((depth, cols), jnp.bfloat16),
                pltpu.VMEM((BOTTOM, cols), jnp.float32),
                pltpu.VMEM((BOTTOM, depth), jnp.bfloat16),
            ),
            in_specs=[hbm, hbm],
            out_specs=(vmem, vmem, vmem, vmem),
            scratch_shapes=[
                pltpu.VMEM((rows - BOTTOM, depth), jnp.bfloat16),
                pltpu.VMEM((rows - BOTTOM, depth), jnp.bfloat16),
                pltpu.VMEM((depth, cols), jnp.bfloat16),
                pltpu.VMEM((rows - BOTTOM, cols), jnp.float32),
                dma,
                dma,
                dma,
                dma((B_PARTS,)),
                dma((B_PARTS,)),
                dma((len(FIRST),)),
                dma((len(FIRST),)),
                pltpu.SemaphoreType.REGULAR,
                pltpu.SemaphoreType.REGULAR,
                pltpu.VMEM(FIRST[AROUND][1::2], jnp.bfloat16),
                dma((3,)),
            ],
            compiler_params=params(collective_id=0, vmem_limit_bytes=40 * 1024 * 1024),
            cost_estimate=pl.CostEstimate(flops=4 * rows * depth * cols, bytes_accessed=12 * depth * cols, transcendentals=0),
        )(a_blk, b_blk)
        written, token = pl.pallas_call(
            write_top,
            out_shape=(c_type, pltpu.VMEM((8, 128), jnp.float32)),
            in_specs=[vmem],
            out_specs=(hbm, vmem),
            scratch_shapes=[dma],
            compiler_params=pltpu.CompilerParams(vmem_limit_bytes=16 * 1024 * 1024),
        )(c_top)
        c_ready, a_far, low_total = pl.pallas_call(
            second_kernel,
            out_shape=(
                pltpu.VMEM((SECOND[-1][0], cols), jnp.bfloat16),
                pltpu.VMEM((BOTTOM, depth), jnp.bfloat16),
                pltpu.VMEM((BOTTOM, cols), jnp.float32),
            ),
            in_specs=[vmem, vmem, vmem, vmem],
            out_specs=(vmem, vmem, vmem),
            scratch_shapes=[
                dma((len(SECOND),)),
                dma((len(SECOND),)),
            ],
            compiler_params=params(collective_id=1, vmem_limit_bytes=16 * 1024 * 1024),
        )(a_low, token, b_far, low)
        return pl.pallas_call(
            write_bottom,
            out_shape=c_type,
            in_specs=[hbm, vmem, vmem, vmem, vmem],
            out_specs=hbm,
            scratch_shapes=[pltpu.VMEM((SECOND[-1][1], cols), jnp.bfloat16), dma, dma((4,))],
            input_output_aliases={0: 0},
            compiler_params=pltpu.CompilerParams(vmem_limit_bytes=16 * 1024 * 1024),
        )(written, c_ready, a_far, low_total, b_far)

    return jax.shard_map(
        local_mm, mesh=mesh, in_specs=(P("row", "col"), P("row", "col")), out_specs=P(("row", "depth"), "col"), check_vma=False
    )
```

```python
import functools

import jax
import jax.numpy as jnp
from jax import lax
from jax.experimental import pallas as pl
from jax.experimental.pallas import tpu as pltpu
from jax.sharding import PartitionSpec as P

MESH = pl.DeviceIdType.MESH
BOTTOM = 192
FIRST = (
    (0, 256, 0, 2048),
    (256, 256, 0, 2048),
    (632, 8, 0, 1792),
    (632, 8, 1792, 256),
    (512, 120, 0, 2048),
    (640, 64, 0, 2048),
    (704, 128, 0, 512),
    (704, 128, 512, 512),
    (704, 128, 1024, 512),
    (704, 128, 1536, 512),
)
SECOND = (
    (0, 192, 0, 1024),
    (0, 192, 1024, 512),
    (0, 192, 1536, 256),
    (0, 128, 1792, 256),
    (128, 64, 1792, 256),
)
AROUND = 2
HOLD = 5
TURN = 6
B_PARTS = 1
TILE_N = 256


def place():
    layer, col, row = lax.axis_index("depth"), lax.axis_index("col"), lax.axis_index("row")
    return layer, col, row, (layer, 1 - col, row), (layer, col, 1 - row), lax.rem(row + col, 2)


def sends_of(pieces, a_src, a_far, send_sem, recv_sem, device):
    return [
        pltpu.make_async_remote_copy(
            src_ref=a_src.at[pl.ds(r0, nr), pl.ds(k0, nk)],
            dst_ref=a_far.at[pl.ds(r0, nr), pl.ds(k0, nk)],
            send_sem=send_sem.at[idx],
            recv_sem=recv_sem.at[idx],
            device_id=device,
            device_id_type=MESH,
        )
        for idx, (r0, nr, k0, nk) in enumerate(pieces)
    ]


def multiply(piece, a_far, b_far, total, c_ref):
    r0, nr, k0, nk = piece
    depth, cols = b_far.shape
    r, k = pl.ds(r0, nr), pl.ds(k0, nk)

    def add(c):
        sums = total[r, c] + jnp.dot(a_far[r, k], b_far[k, c], preferred_element_type=jnp.float32)
        if k0 + nk == depth:
            c_ref[r, c] = sums.astype(c_ref.dtype)
        else:
            total[r, c] = sums

    if nk <= 512:
        for tile in range(4):
            add(pl.ds(tile * (cols // 4), cols // 4))
    else:

        @pl.loop(0, cols // TILE_N)
        def _(tile):
            add(pl.ds(pl.multiple_of(tile * TILE_N, TILE_N), TILE_N))


def first_kernel(
    a_ref,
    b_ref,
    c_ref,
    b_far,
    low,
    a_low,
    a_own,
    a_far,
    b_near,
    total,
    own_sem,
    low_sem,
    bown_sem,
    bsend_sem,
    brecv_sem,
    asend_sem,
    arecv_sem,
    ready_sem,
    turn_sem,
    passing,
    pass_sem,
):
    layer, col, row, across, beside, slot = place()
    top, cols = c_ref.shape
    bottom, depth = a_low.shape
    base = layer * (top + bottom)

    barrier = pltpu.get_barrier_semaphore()
    pl.semaphore_signal(barrier, inc=1, device_id=across, device_id_type=MESH)

    upper = jnp.logical_and(row == 1, layer == 0)
    lower = jnp.logical_and(row == 1, layer == 1)
    below = (1 - layer, col, row)

    @pl.when(row == 1)
    def _():
        pl.semaphore_signal(barrier, inc=1, device_id=beside, device_id_type=MESH)

    @pl.when(upper)
    def _():
        pl.semaphore_signal(barrier, inc=1, device_id=below, device_id_type=MESH)

    @pl.when(lower)
    def _():
        pl.semaphore_wait(barrier, 2)

    @pl.when(upper)
    def _():
        pl.semaphore_wait(barrier, 1)

    @pl.when(row == 0)
    def _():
        pl.semaphore_wait(barrier, 2)
        pl.semaphore_signal(ready_sem, inc=1, device_id=beside, device_id_type=MESH)

    a_sends = sends_of(FIRST, a_own, a_far, asend_sem, arecv_sem, across)
    first_rows = a_ref.at[pl.ds(base, FIRST[0][1]), :]
    a_sends[0] = sends_of(FIRST[:1], first_rows, a_far, asend_sem, arecv_sem, across)[0]
    r0, nr, k0, nk = FIRST[AROUND]
    to_relay = pltpu.make_async_remote_copy(
        src_ref=a_ref.at[pl.ds(r0, nr), pl.ds(k0, nk)],
        dst_ref=passing,
        send_sem=pass_sem.at[0],
        recv_sem=pass_sem.at[1],
        device_id=across,
        device_id_type=MESH,
    )
    from_relay = pltpu.make_async_remote_copy(
        src_ref=passing,
        dst_ref=a_far.at[pl.ds(r0, nr), pl.ds(k0, nk)],
        send_sem=pass_sem.at[2],
        recv_sem=arecv_sem.at[AROUND],
        device_id=below,
        device_id_type=MESH,
    )
    part = depth // B_PARTS

    def sends_of_b(b_buf):
        return [
            pltpu.make_async_remote_copy(
                src_ref=b_ref.at[pl.ds(idx * part, part), :],
                dst_ref=b_buf.at[pl.ds(idx * part, part), :],
                send_sem=bsend_sem.at[idx],
                recv_sem=brecv_sem.at[idx],
                device_id=beside,
                device_id_type=MESH,
            )
            for idx in range(B_PARTS)
        ]

    def own_of_b(b_buf):
        return pltpu.make_async_copy(b_ref, b_buf, bown_sem)

    own_a = pltpu.make_async_copy(a_ref.at[pl.ds(base, top), :], a_own, own_sem)
    own_low = pltpu.make_async_copy(a_ref.at[pl.ds(base + top, bottom), :], a_low, low_sem)

    a_sends[0].start()
    own_a.start()
    own_low.start()
    for value, b_buf in enumerate((b_near, b_far)):

        @pl.when(slot == value)
        def _():
            own_of_b(b_buf).start()

    @pl.when(row == 1)
    def _():
        pl.semaphore_wait(ready_sem, 1)

    for value, b_buf in enumerate((b_near, b_far)):

        @pl.when(slot == value)
        def _():
            for send in sends_of_b(b_buf):
                send.start()

    @pl.when(lower)
    def _():
        to_relay.start()

    for value, (b_mine, b_other) in enumerate(((b_near, b_far), (b_far, b_near))):

        @pl.when(slot == value)
        def _():
            for send in sends_of_b(b_other):
                send.wait_recv()
            own_of_b(b_mine).wait()

    own_a.wait()
    own_low.wait()
    a_sends[1].start()

    @pl.when(jnp.logical_not(upper))
    def _():
        a_sends[AROUND].start()

    for send in a_sends[AROUND + 1 : HOLD]:
        send.start()

    @pl.when(row == 0)
    def _():
        for send in a_sends[HOLD:]:
            send.start()

    col_tiles = cols // TILE_N
    tile_m = top // 4

    @pl.loop(0, 4 * col_tiles)
    def _(tile):
        r = pl.ds(pl.multiple_of((tile // col_tiles) * tile_m, 16), tile_m)
        c = pl.ds(pl.multiple_of((tile % col_tiles) * TILE_N, TILE_N), TILE_N)
        total[r, c] = jnp.dot(a_own[r, :], b_near[:, c], preferred_element_type=jnp.float32)

    @pl.loop(0, col_tiles)
    def _(tile):
        c = pl.ds(pl.multiple_of(tile * TILE_N, TILE_N), TILE_N)
        low[:, c] = jnp.dot(a_low[...], b_near[:, c], preferred_element_type=jnp.float32)

    for idx, piece in enumerate(FIRST):
        if idx == HOLD:

            @pl.when(row == 1)
            def _():
                pl.semaphore_wait(turn_sem, 1)
                for send in a_sends[HOLD:]:
                    send.start()

        a_sends[idx].wait_recv()
        if idx == TURN:

            @pl.when(row == 0)
            def _():
                a_sends[TURN].wait_send()
                pl.semaphore_signal(turn_sem, inc=1, device_id=beside, device_id_type=MESH)

        if idx == AROUND + 2:
            piece = (piece[0], piece[1] + FIRST[AROUND][1], *piece[2:])
        if idx not in (AROUND, AROUND + 1):
            multiply(piece, a_far, b_far, total, c_ref)
        if idx == 0:

            @pl.when(lower)
            def _():
                to_relay.wait_recv()
                from_relay.start()

    for idx, send in enumerate(a_sends):
        if idx not in (TURN, AROUND):
            send.wait_send()

    @pl.when(jnp.logical_not(upper))
    def _():
        a_sends[AROUND].wait_send()

    @pl.when(lower)
    def _():
        to_relay.wait_send()
        from_relay.wait_send()

    @pl.when(row == 1)
    def _():
        a_sends[TURN].wait_send()

    for value, b_buf in enumerate((b_near, b_far)):

        @pl.when(slot == value)
        def _():
            for send in sends_of_b(b_buf):
                send.wait_send()


def second_kernel(a_low, token_ref, b_far, low_ref, c_ref, a_far, total, asend_sem, arecv_sem):
    del token_ref
    _, _, _, across, _, _ = place()

    barrier = pltpu.get_barrier_semaphore()
    pl.semaphore_signal(barrier, inc=1, device_id=across, device_id_type=MESH)
    pl.semaphore_wait(barrier, 1)
    a_sends = sends_of(SECOND, a_low, a_far, asend_sem, arecv_sem, across)
    for send in a_sends:
        send.start()
    total[...] = low_ref[...]
    for idx, piece in enumerate(SECOND):
        a_sends[idx].wait_recv()
        if idx + 1 < len(SECOND):
            multiply(piece, a_far, b_far, total, c_ref)
    for send in a_sends:
        send.wait_send()


def write_top(top_ref, out_ref, token_ref, sem):
    copy = pltpu.make_async_copy(top_ref, out_ref.at[pl.ds(0, top_ref.shape[0]), :], sem)
    copy.start()
    token_ref[...] = jnp.zeros_like(token_ref)
    copy.wait()


def write_bottom(half_ref, ready_ref, a_far, total, b_far, out_ref, last, ready_sem, last_sem):
    del half_ref
    rows, ready = out_ref.shape[0], ready_ref.shape[0]
    r0, nr, k0, nk = SECOND[-1]
    first_row = rows - r0 - nr
    ready_copy = pltpu.make_async_copy(ready_ref, out_ref.at[pl.ds(first_row, ready), :], ready_sem)
    ready_copy.start()
    tn = last.shape[1] // 4
    copies = [ready_copy]
    for tile in range(4):
        r, k, c = pl.ds(r0, nr), pl.ds(k0, nk), pl.ds(tile * tn, tn)
        sums = total[r, c] + jnp.dot(a_far[r, k], b_far[k, c], preferred_element_type=jnp.float32)
        last[:, c] = sums.astype(last.dtype)
        copies.append(pltpu.make_async_copy(last.at[:, c], out_ref.at[pl.ds(first_row + r0, nr), c], last_sem.at[tile]))
        copies[-1].start()
    for copy in copies:
        copy.wait()


def solution(mesh):
    depth_n = mesh.shape["depth"]
    dma = pltpu.SemaphoreType.DMA
    hbm, vmem = pl.BlockSpec(memory_space=pltpu.HBM), pl.BlockSpec(memory_space=pltpu.VMEM)

    def local_mm(a_blk, b_blk):
        rows = a_blk.shape[0] // depth_n
        depth, cols = b_blk.shape
        c_type = jax.ShapeDtypeStruct((rows, cols), jnp.bfloat16)
        params = functools.partial(pltpu.CompilerParams, has_side_effects=True)
        c_top, b_far, low, a_low = pl.pallas_call(
            first_kernel,
            out_shape=(
                pltpu.VMEM((rows - BOTTOM, cols), jnp.bfloat16),
                pltpu.VMEM((depth, cols), jnp.bfloat16),
                pltpu.VMEM((BOTTOM, cols), jnp.float32),
                pltpu.VMEM((BOTTOM, depth), jnp.bfloat16),
            ),
            in_specs=[hbm, hbm],
            out_specs=(vmem, vmem, vmem, vmem),
            scratch_shapes=[
                pltpu.VMEM((rows - BOTTOM, depth), jnp.bfloat16),
                pltpu.VMEM((rows - BOTTOM, depth), jnp.bfloat16),
                pltpu.VMEM((depth, cols), jnp.bfloat16),
                pltpu.VMEM((rows - BOTTOM, cols), jnp.float32),
                dma,
                dma,
                dma,
                dma((B_PARTS,)),
                dma((B_PARTS,)),
                dma((len(FIRST),)),
                dma((len(FIRST),)),
                pltpu.SemaphoreType.REGULAR,
                pltpu.SemaphoreType.REGULAR,
                pltpu.VMEM(FIRST[AROUND][1::2], jnp.bfloat16),
                dma((3,)),
            ],
            compiler_params=params(collective_id=0, vmem_limit_bytes=40 * 1024 * 1024),
            cost_estimate=pl.CostEstimate(flops=4 * rows * depth * cols, bytes_accessed=12 * depth * cols, transcendentals=0),
        )(a_blk, b_blk)
        written, token = pl.pallas_call(
            write_top,
            out_shape=(c_type, pltpu.VMEM((8, 128), jnp.float32)),
            in_specs=[vmem],
            out_specs=(hbm, vmem),
            scratch_shapes=[dma],
            compiler_params=pltpu.CompilerParams(vmem_limit_bytes=16 * 1024 * 1024),
        )(c_top)
        c_ready, a_far, low_total = pl.pallas_call(
            second_kernel,
            out_shape=(
                pltpu.VMEM((SECOND[-1][0], cols), jnp.bfloat16),
                pltpu.VMEM((BOTTOM, depth), jnp.bfloat16),
                pltpu.VMEM((BOTTOM, cols), jnp.float32),
            ),
            in_specs=[vmem, vmem, vmem, vmem],
            out_specs=(vmem, vmem, vmem),
            scratch_shapes=[
                dma((len(SECOND),)),
                dma((len(SECOND),)),
            ],
            compiler_params=params(collective_id=1, vmem_limit_bytes=16 * 1024 * 1024),
        )(a_low, token, b_far, low)
        return pl.pallas_call(
            write_bottom,
            out_shape=c_type,
            in_specs=[hbm, vmem, vmem, vmem, vmem],
            out_specs=hbm,
            scratch_shapes=[pltpu.VMEM((SECOND[-1][1], cols), jnp.bfloat16), dma, dma((4,))],
            input_output_aliases={0: 0},
            compiler_params=pltpu.CompilerParams(vmem_limit_bytes=16 * 1024 * 1024),
        )(written, c_ready, a_far, low_total, b_far)

    return jax.shard_map(
        local_mm, mesh=mesh, in_specs=(P("row", "col"), P("row", "col")), out_specs=P(("row", "depth"), "col"), check_vma=False
    )
```

```python
import functools

import jax
import jax.numpy as jnp
from jax import lax
from jax.experimental import pallas as pl
from jax.experimental.pallas import tpu as pltpu
from jax.sharding import PartitionSpec as P

MESH = pl.DeviceIdType.MESH
BOTTOM = 192
FIRST = (
    (0, 128, 0, 2048),
    (128, 384, 0, 2048),
    (632, 8, 0, 1792),
    (632, 8, 1792, 256),
    (512, 120, 0, 2048),
    (640, 64, 0, 2048),
    (704, 128, 0, 512),
    (704, 128, 512, 512),
    (704, 128, 1024, 512),
    (704, 128, 1536, 512),
)
SECOND = (
    (0, 192, 0, 1024),
    (0, 192, 1024, 512),
    (0, 192, 1536, 256),
    (0, 128, 1792, 256),
    (128, 64, 1792, 256),
)
AROUND = 2
HOLD = 5
TURN = 6
TILE_N = 256


def place():
    layer, col, row = lax.axis_index("depth"), lax.axis_index("col"), lax.axis_index("row")
    return layer, col, row, (layer, 1 - col, row), (layer, col, 1 - row), lax.rem(row + col, 2)


def sends_of(pieces, a_src, a_far, send_sem, recv_sem, device):
    return [
        pltpu.make_async_remote_copy(
            src_ref=a_src.at[pl.ds(r0, nr), pl.ds(k0, nk)],
            dst_ref=a_far.at[pl.ds(r0, nr), pl.ds(k0, nk)],
            send_sem=send_sem.at[idx],
            recv_sem=recv_sem.at[idx],
            device_id=device,
            device_id_type=MESH,
        )
        for idx, (r0, nr, k0, nk) in enumerate(pieces)
    ]


def multiply(piece, a_far, b_far, total, c_ref):
    r0, nr, k0, nk = piece
    depth, cols = b_far.shape
    r, k = pl.ds(r0, nr), pl.ds(k0, nk)

    def add(c):
        sums = total[r, c] + jnp.dot(a_far[r, k], b_far[k, c], preferred_element_type=jnp.float32)
        if k0 + nk == depth:
            c_ref[r, c] = sums.astype(c_ref.dtype)
        else:
            total[r, c] = sums

    if nk <= 512:
        for tile in range(4):
            add(pl.ds(tile * (cols // 4), cols // 4))
    else:

        @pl.loop(0, cols // TILE_N)
        def _(tile):
            add(pl.ds(pl.multiple_of(tile * TILE_N, TILE_N), TILE_N))


def first_kernel(
    a_ref,
    b_ref,
    c_ref,
    b_far,
    low,
    a_low,
    a_own,
    a_far,
    b_near,
    total,
    own_sem,
    low_sem,
    bown_sem,
    bsend_sem,
    brecv_sem,
    asend_sem,
    arecv_sem,
    ready_sem,
    turn_sem,
    passing,
    pass_sem,
):
    layer, col, row, across, beside, slot = place()
    top, cols = c_ref.shape
    bottom, depth = a_low.shape
    base = layer * (top + bottom)

    barrier = pltpu.get_barrier_semaphore()
    pl.semaphore_signal(barrier, inc=1, device_id=across, device_id_type=MESH)

    upper = jnp.logical_and(row == 1, layer == 0)
    lower = jnp.logical_and(row == 1, layer == 1)
    below = (1 - layer, col, row)

    @pl.when(row == 1)
    def _():
        pl.semaphore_signal(barrier, inc=1, device_id=beside, device_id_type=MESH)

    @pl.when(upper)
    def _():
        pl.semaphore_signal(barrier, inc=1, device_id=below, device_id_type=MESH)

    @pl.when(lower)
    def _():
        pl.semaphore_wait(barrier, 2)

    @pl.when(upper)
    def _():
        pl.semaphore_wait(barrier, 1)

    @pl.when(row == 0)
    def _():
        pl.semaphore_wait(barrier, 2)
        pl.semaphore_signal(ready_sem, inc=1, device_id=beside, device_id_type=MESH)

    a_sends = sends_of(FIRST, a_own, a_far, asend_sem, arecv_sem, across)
    first_rows = a_ref.at[pl.ds(base, top), :]
    a_sends[:AROUND] = sends_of(FIRST[:AROUND], first_rows, a_far, asend_sem, arecv_sem, across)
    r0, nr, k0, nk = FIRST[AROUND]
    to_relay = pltpu.make_async_remote_copy(
        src_ref=a_ref.at[pl.ds(r0, nr), pl.ds(k0, nk)],
        dst_ref=passing,
        send_sem=pass_sem.at[0],
        recv_sem=pass_sem.at[1],
        device_id=across,
        device_id_type=MESH,
    )
    from_relay = pltpu.make_async_remote_copy(
        src_ref=passing,
        dst_ref=a_far.at[pl.ds(r0, nr), pl.ds(k0, nk)],
        send_sem=pass_sem.at[2],
        recv_sem=arecv_sem.at[AROUND],
        device_id=below,
        device_id_type=MESH,
    )
    own_a = pltpu.make_async_copy(a_ref.at[pl.ds(base, top), :], a_own, own_sem)
    own_low = pltpu.make_async_copy(a_ref.at[pl.ds(base + top, bottom), :], a_low, low_sem)

    def own_of_b(b_buf):
        return pltpu.make_async_copy(b_ref, b_buf, bown_sem)

    def send_of_b(b_buf):
        return pltpu.make_async_remote_copy(
            src_ref=b_buf,
            dst_ref=b_buf,
            send_sem=bsend_sem,
            recv_sem=brecv_sem,
            device_id=beside,
            device_id_type=MESH,
        )

    a_sends[0].start()

    @pl.when(lower)
    def _():
        to_relay.start()

    for send in a_sends[1:AROUND]:
        send.start()

    own_a.start()
    own_low.start()
    for value, b_buf in enumerate((b_near, b_far)):

        @pl.when(slot == value)
        def _():
            own_of_b(b_buf).start()

    @pl.when(row == 1)
    def _():
        pl.semaphore_wait(ready_sem, 1)

    a_sends[0].wait_recv()
    own_a.wait()
    own_low.wait()
    for value, b_buf in enumerate((b_near, b_far)):

        @pl.when(slot == value)
        def _():
            own_of_b(b_buf).wait()
            send_of_b(b_buf).start()

    @pl.when(jnp.logical_not(upper))
    def _():
        a_sends[AROUND].start()

    for send in a_sends[AROUND + 1 : HOLD]:
        send.start()

    @pl.when(row == 0)
    def _():
        for send in a_sends[HOLD:]:
            send.start()

    @pl.when(lower)
    def _():
        to_relay.wait_recv()
        from_relay.start()

    for value, b_buf in enumerate((b_far, b_near)):

        @pl.when(slot == value)
        def _():
            send_of_b(b_buf).wait_recv()

    col_tiles = cols // TILE_N
    tile_m = top // 4

    @pl.loop(0, 4 * col_tiles)
    def _(tile):
        r = pl.ds(pl.multiple_of((tile // col_tiles) * tile_m, 16), tile_m)
        c = pl.ds(pl.multiple_of((tile % col_tiles) * TILE_N, TILE_N), TILE_N)
        total[r, c] = jnp.dot(a_own[r, :], b_near[:, c], preferred_element_type=jnp.float32)

    @pl.loop(0, col_tiles)
    def _(tile):
        c = pl.ds(pl.multiple_of(tile * TILE_N, TILE_N), TILE_N)
        low[:, c] = jnp.dot(a_low[...], b_near[:, c], preferred_element_type=jnp.float32)

    for idx, piece in enumerate(FIRST):
        if idx == HOLD:

            @pl.when(row == 1)
            def _():
                pl.semaphore_wait(turn_sem, 1)
                for send in a_sends[HOLD:]:
                    send.start()

        if idx:
            a_sends[idx].wait_recv()
        if idx == TURN:

            @pl.when(row == 0)
            def _():
                a_sends[TURN].wait_send()
                pl.semaphore_signal(turn_sem, inc=1, device_id=beside, device_id_type=MESH)

        if idx == AROUND + 2:
            piece = (piece[0], piece[1] + FIRST[AROUND][1], *piece[2:])
        if idx not in (AROUND, AROUND + 1):
            multiply(piece, a_far, b_far, total, c_ref)
    for idx, send in enumerate(a_sends):
        if idx not in (TURN, AROUND):
            send.wait_send()

    @pl.when(jnp.logical_not(upper))
    def _():
        a_sends[AROUND].wait_send()

    @pl.when(lower)
    def _():
        to_relay.wait_send()
        from_relay.wait_send()

    @pl.when(row == 1)
    def _():
        a_sends[TURN].wait_send()

    for value, b_buf in enumerate((b_near, b_far)):

        @pl.when(slot == value)
        def _():
            send_of_b(b_buf).wait_send()


def second_kernel(a_low, token_ref, b_far, low_ref, c_ref, a_far, total, asend_sem, arecv_sem):
    del token_ref
    _, _, _, across, _, _ = place()

    barrier = pltpu.get_barrier_semaphore()
    pl.semaphore_signal(barrier, inc=1, device_id=across, device_id_type=MESH)
    pl.semaphore_wait(barrier, 1)
    a_sends = sends_of(SECOND, a_low, a_far, asend_sem, arecv_sem, across)
    for send in a_sends:
        send.start()
    total[...] = low_ref[...]
    for idx, piece in enumerate(SECOND):
        a_sends[idx].wait_recv()
        if idx + 1 < len(SECOND):
            multiply(piece, a_far, b_far, total, c_ref)
    for send in a_sends:
        send.wait_send()


def write_top(top_ref, out_ref, token_ref, sem):
    copy = pltpu.make_async_copy(top_ref, out_ref.at[pl.ds(0, top_ref.shape[0]), :], sem)
    copy.start()
    token_ref[...] = jnp.zeros_like(token_ref)
    copy.wait()


def write_bottom(half_ref, ready_ref, a_far, total, b_far, out_ref, last, ready_sem, last_sem):
    del half_ref
    rows, ready = out_ref.shape[0], ready_ref.shape[0]
    r0, nr, k0, nk = SECOND[-1]
    first_row = rows - r0 - nr
    ready_copy = pltpu.make_async_copy(ready_ref, out_ref.at[pl.ds(first_row, ready), :], ready_sem)
    ready_copy.start()
    tn = last.shape[1] // 4
    copies = [ready_copy]
    for tile in range(4):
        r, k, c = pl.ds(r0, nr), pl.ds(k0, nk), pl.ds(tile * tn, tn)
        sums = total[r, c] + jnp.dot(a_far[r, k], b_far[k, c], preferred_element_type=jnp.float32)
        last[:, c] = sums.astype(last.dtype)
        copies.append(pltpu.make_async_copy(last.at[:, c], out_ref.at[pl.ds(first_row + r0, nr), c], last_sem.at[tile]))
        copies[-1].start()
    for copy in copies:
        copy.wait()


def solution(mesh):
    depth_n = mesh.shape["depth"]
    dma = pltpu.SemaphoreType.DMA
    hbm, vmem = pl.BlockSpec(memory_space=pltpu.HBM), pl.BlockSpec(memory_space=pltpu.VMEM)

    def local_mm(a_blk, b_blk):
        rows = a_blk.shape[0] // depth_n
        depth, cols = b_blk.shape
        c_type = jax.ShapeDtypeStruct((rows, cols), jnp.bfloat16)
        params = functools.partial(pltpu.CompilerParams, has_side_effects=True)
        c_top, b_far, low, a_low = pl.pallas_call(
            first_kernel,
            out_shape=(
                pltpu.VMEM((rows - BOTTOM, cols), jnp.bfloat16),
                pltpu.VMEM((depth, cols), jnp.bfloat16),
                pltpu.VMEM((BOTTOM, cols), jnp.float32),
                pltpu.VMEM((BOTTOM, depth), jnp.bfloat16),
            ),
            in_specs=[hbm, hbm],
            out_specs=(vmem, vmem, vmem, vmem),
            scratch_shapes=[
                pltpu.VMEM((rows - BOTTOM, depth), jnp.bfloat16),
                pltpu.VMEM((rows - BOTTOM, depth), jnp.bfloat16),
                pltpu.VMEM((depth, cols), jnp.bfloat16),
                pltpu.VMEM((rows - BOTTOM, cols), jnp.float32),
                dma,
                dma,
                dma,
                dma,
                dma,
                dma((len(FIRST),)),
                dma((len(FIRST),)),
                pltpu.SemaphoreType.REGULAR,
                pltpu.SemaphoreType.REGULAR,
                pltpu.VMEM(FIRST[AROUND][1::2], jnp.bfloat16),
                dma((3,)),
            ],
            compiler_params=params(collective_id=0, vmem_limit_bytes=40 * 1024 * 1024),
            cost_estimate=pl.CostEstimate(flops=4 * rows * depth * cols, bytes_accessed=12 * depth * cols, transcendentals=0),
        )(a_blk, b_blk)
        written, token = pl.pallas_call(
            write_top,
            out_shape=(c_type, pltpu.VMEM((8, 128), jnp.float32)),
            in_specs=[vmem],
            out_specs=(hbm, vmem),
            scratch_shapes=[dma],
            compiler_params=pltpu.CompilerParams(vmem_limit_bytes=16 * 1024 * 1024),
        )(c_top)
        c_ready, a_far, low_total = pl.pallas_call(
            second_kernel,
            out_shape=(
                pltpu.VMEM((SECOND[-1][0], cols), jnp.bfloat16),
                pltpu.VMEM((BOTTOM, depth), jnp.bfloat16),
                pltpu.VMEM((BOTTOM, cols), jnp.float32),
            ),
            in_specs=[vmem, vmem, vmem, vmem],
            out_specs=(vmem, vmem, vmem),
            scratch_shapes=[
                dma((len(SECOND),)),
                dma((len(SECOND),)),
            ],
            compiler_params=params(collective_id=1, vmem_limit_bytes=16 * 1024 * 1024),
        )(a_low, token, b_far, low)
        return pl.pallas_call(
            write_bottom,
            out_shape=c_type,
            in_specs=[hbm, vmem, vmem, vmem, vmem],
            out_specs=hbm,
            scratch_shapes=[pltpu.VMEM((SECOND[-1][1], cols), jnp.bfloat16), dma, dma((4,))],
            input_output_aliases={0: 0},
            compiler_params=pltpu.CompilerParams(vmem_limit_bytes=16 * 1024 * 1024),
        )(written, c_ready, a_far, low_total, b_far)

    return jax.shard_map(
        local_mm, mesh=mesh, in_specs=(P("row", "col"), P("row", "col")), out_specs=P(("row", "depth"), "col"), check_vma=False
    )
```

```python
import functools

import jax
import jax.numpy as jnp
from jax import lax
from jax.experimental import pallas as pl
from jax.experimental.pallas import tpu as pltpu
from jax.sharding import PartitionSpec as P

MESH = pl.DeviceIdType.MESH
BOTTOM = 192
FIRST = (
    (0, 128, 0, 2048),
    (128, 384, 0, 2048),
    (584, 8, 0, 1664),
    (584, 8, 1664, 384),
    (512, 72, 0, 2048),
    (592, 112, 0, 2048),
    (704, 128, 0, 1024),
    (704, 128, 1024, 512),
    (704, 128, 1536, 512),
)
SECOND = (
    (0, 192, 0, 1024),
    (0, 192, 1024, 512),
    (0, 192, 1536, 256),
    (0, 128, 1792, 256),
    (128, 64, 1792, 256),
)
AROUND = 2
HOLD = 5
TURN = 5
TILE_N = 256


def place():
    layer, col, row = lax.axis_index("depth"), lax.axis_index("col"), lax.axis_index("row")
    return layer, col, row, (layer, 1 - col, row), (layer, col, 1 - row), lax.rem(row + col, 2)


def sends_of(pieces, a_src, a_far, send_sem, recv_sem, device):
    return [
        pltpu.make_async_remote_copy(
            src_ref=a_src.at[pl.ds(r0, nr), pl.ds(k0, nk)],
            dst_ref=a_far.at[pl.ds(r0, nr), pl.ds(k0, nk)],
            send_sem=send_sem.at[idx],
            recv_sem=recv_sem.at[idx],
            device_id=device,
            device_id_type=MESH,
        )
        for idx, (r0, nr, k0, nk) in enumerate(pieces)
    ]


def multiply(piece, a_far, b_far, total, c_ref):
    r0, nr, k0, nk = piece
    depth, cols = b_far.shape
    r, k = pl.ds(r0, nr), pl.ds(k0, nk)

    def add(c):
        sums = total[r, c] + jnp.dot(a_far[r, k], b_far[k, c], preferred_element_type=jnp.float32)
        if k0 + nk == depth:
            c_ref[r, c] = sums.astype(c_ref.dtype)
        else:
            total[r, c] = sums

    if nk <= 512:
        for tile in range(4):
            add(pl.ds(tile * (cols // 4), cols // 4))
    else:

        @pl.loop(0, cols // TILE_N)
        def _(tile):
            add(pl.ds(pl.multiple_of(tile * TILE_N, TILE_N), TILE_N))


def first_kernel(
    a_ref,
    b_ref,
    c_ref,
    b_far,
    low,
    a_low,
    a_own,
    a_far,
    b_near,
    total,
    own_sem,
    low_sem,
    bown_sem,
    bsend_sem,
    brecv_sem,
    asend_sem,
    arecv_sem,
    ready_sem,
    turn_sem,
    passing,
    pass_sem,
):
    layer, col, row, across, beside, slot = place()
    top, cols = c_ref.shape
    bottom, depth = a_low.shape
    base = layer * (top + bottom)

    barrier = pltpu.get_barrier_semaphore()
    pl.semaphore_signal(barrier, inc=1, device_id=across, device_id_type=MESH)

    upper = jnp.logical_and(row == 1, layer == 0)
    lower = jnp.logical_and(row == 1, layer == 1)
    below = (1 - layer, col, row)

    @pl.when(row == 1)
    def _():
        pl.semaphore_signal(barrier, inc=1, device_id=beside, device_id_type=MESH)

    @pl.when(upper)
    def _():
        pl.semaphore_signal(barrier, inc=1, device_id=below, device_id_type=MESH)

    @pl.when(lower)
    def _():
        pl.semaphore_wait(barrier, 2)

    @pl.when(upper)
    def _():
        pl.semaphore_wait(barrier, 1)

    @pl.when(row == 0)
    def _():
        pl.semaphore_wait(barrier, 2)
        pl.semaphore_signal(ready_sem, inc=1, device_id=beside, device_id_type=MESH)

    a_sends = sends_of(FIRST, a_own, a_far, asend_sem, arecv_sem, across)
    first_rows = a_ref.at[pl.ds(base, top), :]
    a_sends[:AROUND] = sends_of(FIRST[:AROUND], first_rows, a_far, asend_sem, arecv_sem, across)
    r0, nr, k0, nk = FIRST[AROUND]
    to_relay = pltpu.make_async_remote_copy(
        src_ref=a_ref.at[pl.ds(r0, nr), pl.ds(k0, nk)],
        dst_ref=passing,
        send_sem=pass_sem.at[0],
        recv_sem=pass_sem.at[1],
        device_id=across,
        device_id_type=MESH,
    )
    from_relay = pltpu.make_async_remote_copy(
        src_ref=passing,
        dst_ref=a_far.at[pl.ds(r0, nr), pl.ds(k0, nk)],
        send_sem=pass_sem.at[2],
        recv_sem=arecv_sem.at[AROUND],
        device_id=below,
        device_id_type=MESH,
    )
    own_a = pltpu.make_async_copy(a_ref.at[pl.ds(base, top), :], a_own, own_sem)
    own_low = pltpu.make_async_copy(a_ref.at[pl.ds(base + top, bottom), :], a_low, low_sem)

    def own_of_b(b_buf):
        return pltpu.make_async_copy(b_ref, b_buf, bown_sem)

    def send_of_b(b_buf):
        return pltpu.make_async_remote_copy(
            src_ref=b_buf,
            dst_ref=b_buf,
            send_sem=bsend_sem,
            recv_sem=brecv_sem,
            device_id=beside,
            device_id_type=MESH,
        )

    a_sends[0].start()

    @pl.when(lower)
    def _():
        to_relay.start()

    for send in a_sends[1:AROUND]:
        send.start()

    own_a.start()
    own_low.start()
    for value, b_buf in enumerate((b_near, b_far)):

        @pl.when(slot == value)
        def _():
            own_of_b(b_buf).start()

    @pl.when(row == 1)
    def _():
        pl.semaphore_wait(ready_sem, 1)

    a_sends[0].wait_recv()
    own_a.wait()
    own_low.wait()
    for value, b_buf in enumerate((b_near, b_far)):

        @pl.when(slot == value)
        def _():
            own_of_b(b_buf).wait()
            send_of_b(b_buf).start()

    @pl.when(jnp.logical_not(upper))
    def _():
        a_sends[AROUND].start()

    for send in a_sends[AROUND + 1 : HOLD]:
        send.start()

    @pl.when(row == 0)
    def _():
        for send in a_sends[HOLD:]:
            send.start()

    @pl.when(lower)
    def _():
        to_relay.wait_recv()
        from_relay.start()

    for value, b_buf in enumerate((b_far, b_near)):

        @pl.when(slot == value)
        def _():
            send_of_b(b_buf).wait_recv()

    col_tiles = cols // TILE_N
    tile_m = top // 4

    @pl.loop(0, 4 * col_tiles)
    def _(tile):
        r = pl.ds(pl.multiple_of((tile // col_tiles) * tile_m, 16), tile_m)
        c = pl.ds(pl.multiple_of((tile % col_tiles) * TILE_N, TILE_N), TILE_N)
        total[r, c] = jnp.dot(a_own[r, :], b_near[:, c], preferred_element_type=jnp.float32)

    @pl.loop(0, col_tiles)
    def _(tile):
        c = pl.ds(pl.multiple_of(tile * TILE_N, TILE_N), TILE_N)
        low[:, c] = jnp.dot(a_low[...], b_near[:, c], preferred_element_type=jnp.float32)

    for idx, piece in enumerate(FIRST):
        if idx == HOLD:

            @pl.when(row == 1)
            def _():
                pl.semaphore_wait(turn_sem, 1)
                for send in a_sends[HOLD:]:
                    send.start()

        if idx:
            a_sends[idx].wait_recv()
        if idx == TURN:

            @pl.when(row == 0)
            def _():
                a_sends[TURN].wait_send()
                pl.semaphore_signal(turn_sem, inc=1, device_id=beside, device_id_type=MESH)

        if idx == AROUND + 2:
            piece = (piece[0], piece[1] + FIRST[AROUND][1], *piece[2:])
        if idx not in (AROUND, AROUND + 1):
            multiply(piece, a_far, b_far, total, c_ref)
    for idx, send in enumerate(a_sends):
        if idx not in (TURN, AROUND):
            send.wait_send()

    @pl.when(jnp.logical_not(upper))
    def _():
        a_sends[AROUND].wait_send()

    @pl.when(lower)
    def _():
        to_relay.wait_send()
        from_relay.wait_send()

    @pl.when(row == 1)
    def _():
        a_sends[TURN].wait_send()

    for value, b_buf in enumerate((b_near, b_far)):

        @pl.when(slot == value)
        def _():
            send_of_b(b_buf).wait_send()


def second_kernel(a_low, token_ref, b_far, low_ref, c_ref, a_far, total, asend_sem, arecv_sem):
    del token_ref
    _, _, _, across, _, _ = place()

    barrier = pltpu.get_barrier_semaphore()
    pl.semaphore_signal(barrier, inc=1, device_id=across, device_id_type=MESH)
    pl.semaphore_wait(barrier, 1)
    a_sends = sends_of(SECOND, a_low, a_far, asend_sem, arecv_sem, across)
    for send in a_sends:
        send.start()
    total[...] = low_ref[...]
    for idx, piece in enumerate(SECOND):
        a_sends[idx].wait_recv()
        if idx + 1 < len(SECOND):
            multiply(piece, a_far, b_far, total, c_ref)
    for send in a_sends:
        send.wait_send()


def write_top(top_ref, out_ref, token_ref, sem):
    copy = pltpu.make_async_copy(top_ref, out_ref.at[pl.ds(0, top_ref.shape[0]), :], sem)
    copy.start()
    token_ref[...] = jnp.zeros_like(token_ref)
    copy.wait()


def write_bottom(half_ref, ready_ref, a_far, total, b_far, out_ref, last, ready_sem, last_sem):
    del half_ref
    rows, ready = out_ref.shape[0], ready_ref.shape[0]
    r0, nr, k0, nk = SECOND[-1]
    first_row = rows - r0 - nr
    ready_copy = pltpu.make_async_copy(ready_ref, out_ref.at[pl.ds(first_row, ready), :], ready_sem)
    ready_copy.start()
    tn = last.shape[1] // 4
    copies = [ready_copy]
    for tile in range(4):
        r, k, c = pl.ds(r0, nr), pl.ds(k0, nk), pl.ds(tile * tn, tn)
        sums = total[r, c] + jnp.dot(a_far[r, k], b_far[k, c], preferred_element_type=jnp.float32)
        last[:, c] = sums.astype(last.dtype)
        copies.append(pltpu.make_async_copy(last.at[:, c], out_ref.at[pl.ds(first_row + r0, nr), c], last_sem.at[tile]))
        copies[-1].start()
    for copy in copies:
        copy.wait()


def solution(mesh):
    depth_n = mesh.shape["depth"]
    dma = pltpu.SemaphoreType.DMA
    hbm, vmem = pl.BlockSpec(memory_space=pltpu.HBM), pl.BlockSpec(memory_space=pltpu.VMEM)

    def local_mm(a_blk, b_blk):
        rows = a_blk.shape[0] // depth_n
        depth, cols = b_blk.shape
        c_type = jax.ShapeDtypeStruct((rows, cols), jnp.bfloat16)
        params = functools.partial(pltpu.CompilerParams, has_side_effects=True)
        c_top, b_far, low, a_low = pl.pallas_call(
            first_kernel,
            out_shape=(
                pltpu.VMEM((rows - BOTTOM, cols), jnp.bfloat16),
                pltpu.VMEM((depth, cols), jnp.bfloat16),
                pltpu.VMEM((BOTTOM, cols), jnp.float32),
                pltpu.VMEM((BOTTOM, depth), jnp.bfloat16),
            ),
            in_specs=[hbm, hbm],
            out_specs=(vmem, vmem, vmem, vmem),
            scratch_shapes=[
                pltpu.VMEM((rows - BOTTOM, depth), jnp.bfloat16),
                pltpu.VMEM((rows - BOTTOM, depth), jnp.bfloat16),
                pltpu.VMEM((depth, cols), jnp.bfloat16),
                pltpu.VMEM((rows - BOTTOM, cols), jnp.float32),
                dma,
                dma,
                dma,
                dma,
                dma,
                dma((len(FIRST),)),
                dma((len(FIRST),)),
                pltpu.SemaphoreType.REGULAR,
                pltpu.SemaphoreType.REGULAR,
                pltpu.VMEM(FIRST[AROUND][1::2], jnp.bfloat16),
                dma((3,)),
            ],
            compiler_params=params(collective_id=0, vmem_limit_bytes=40 * 1024 * 1024),
            cost_estimate=pl.CostEstimate(flops=4 * rows * depth * cols, bytes_accessed=12 * depth * cols, transcendentals=0),
        )(a_blk, b_blk)
        written, token = pl.pallas_call(
            write_top,
            out_shape=(c_type, pltpu.VMEM((8, 128), jnp.float32)),
            in_specs=[vmem],
            out_specs=(hbm, vmem),
            scratch_shapes=[dma],
            compiler_params=pltpu.CompilerParams(vmem_limit_bytes=16 * 1024 * 1024),
        )(c_top)
        c_ready, a_far, low_total = pl.pallas_call(
            second_kernel,
            out_shape=(
                pltpu.VMEM((SECOND[-1][0], cols), jnp.bfloat16),
                pltpu.VMEM((BOTTOM, depth), jnp.bfloat16),
                pltpu.VMEM((BOTTOM, cols), jnp.float32),
            ),
            in_specs=[vmem, vmem, vmem, vmem],
            out_specs=(vmem, vmem, vmem),
            scratch_shapes=[
                dma((len(SECOND),)),
                dma((len(SECOND),)),
            ],
            compiler_params=params(collective_id=1, vmem_limit_bytes=16 * 1024 * 1024),
        )(a_low, token, b_far, low)
        return pl.pallas_call(
            write_bottom,
            out_shape=c_type,
            in_specs=[hbm, vmem, vmem, vmem, vmem],
            out_specs=hbm,
            scratch_shapes=[pltpu.VMEM((SECOND[-1][1], cols), jnp.bfloat16), dma, dma((4,))],
            input_output_aliases={0: 0},
            compiler_params=pltpu.CompilerParams(vmem_limit_bytes=16 * 1024 * 1024),
        )(written, c_ready, a_far, low_total, b_far)

    return jax.shard_map(
        local_mm, mesh=mesh, in_specs=(P("row", "col"), P("row", "col")), out_specs=P(("row", "depth"), "col"), check_vma=False
    )
```
